512 devices in a mesh: lat: 64 (over x, z, core), chan: 8 (over y).
Axes of the slice: x: 4, y: 8, z: 8, core: 2. Of those that a mesh axis runs over, the one named last changes fastest.
Arguments:
- spec_in: bfloat16 [384, 1, 256, 2, 384], P('lat', None, 'chan'), may hold values from -6 to 6
- legendre: float32 [384, 384, 384], P('lat'), may hold values from -0.4375 to 0.4375
- mode_slot: int32 [384], replicated, may hold values from 0 to 383, each once
- w_in: bfloat16 [512, 256], replicated, may hold values from -0.375 to 0.375
- b_in: float32 [512], replicated, may hold values from -3 to 3
- w_out: bfloat16 [256, 512], replicated, may hold values from -0.25 to 0.25
- kernel: float32 [256, 9], P('chan'), may hold values from -4 to 4
Outputs:
- spec_out: bfloat16 [384, 1, 256, 2, 384], P('lat', None, 'chan')
The draws below stay inside these ranges and needn't reach their ends.
Inputs may be any that keep to these rules, and one draw needn't show every extreme that they name: mode_slot holds every number of 0 to 383 once.
All inputs are finite; a program needn't handle non-finite values.
Results may differ from the reference program's by a relative error of at most 0.0083.
Values may be sent and summed in bfloat16 or wider, within the bound.
A program may use at most 64 MiB of HBM per device.

```python
import math
import jax
import jax.numpy as jnp
from jax import lax

C = 256
H = 512
NLAT = 384
NLON = 768
M = 384
L = 384
B = 1


def steps_of(rng, shape, pieces, low, high):
    gain, own = 1.0, jax.random.fold_in(rng, 6)
    for axis_at, parts in pieces:
        draws = jnp.exp(jax.random.uniform(jax.random.fold_in(own, axis_at), (parts,), jnp.float32, low / len(pieces), high / len(pieces)))
        gain = gain * jnp.repeat(draws, shape[axis_at] // parts).reshape([-1 if axis == axis_at else 1 for axis in range(len(shape))])
    return gain


def scatter_about(key, extent, deviation, most, pieces=(), kind=jnp.bfloat16):
    drawn = deviation * jax.random.normal(key, extent, jnp.float32)
    if pieces:
        drawn = drawn * steps_of(key, extent, pieces, -0.22, 0.18)
    return jnp.clip(drawn, -most, most).astype(kind)


def setup_inputs(seed: int = 0) -> dict:
    key_list = jax.random.split(jax.random.key(seed), 8)
    spec_in = scatter_about(key_list[0], (M, B, C, 2, L), 1.0, 6.0, ((0, 64), (2, 8)))
    legendre = scatter_about(key_list[1], (M, NLAT, L), (L // 2) ** -0.5, 0.4375, ((0, 64),), jnp.float32)
    mode_slot = jax.random.permutation(key_list[2], M).astype(jnp.int32)
    w_in = scatter_about(key_list[3], (H, C), C ** -0.5, 0.375)
    b_in = scatter_about(key_list[4], (H,), 0.5, 3.0, (), jnp.float32)
    w_out = scatter_about(key_list[5], (C, H), H ** -0.5, 0.25)
    kernel = scatter_about(key_list[6], (C, 9), 0.3, 4.0, ((0, 8),), jnp.float32)
    return {"spec_in": spec_in, "legendre": legendre, "mode_slot": mode_slot, "w_in": w_in, "b_in": b_in, "w_out": w_out, "kernel": kernel}


def wave_table(modes, count):
    columns = jnp.arange(count, dtype=jnp.int32)
    phase = (modes[:, None] * columns[None, :]) % count
    angle = phase.astype(jnp.float32) * (2.0 * math.pi / count)
    factor = count ** -0.5
    return jnp.stack([jnp.cos(angle) * factor, -jnp.sin(angle) * factor], axis=1)


def reference(spec_in, legendre, mode_slot, w_in, b_in, w_out, kernel):
    high = lax.Precision.HIGHEST
    degrees = jnp.arange(L, dtype=jnp.int32)
    masked = jnp.where(degrees[None, None, :] >= mode_slot[:, None, None], legendre, jnp.float32(0.0))
    waves = wave_table(mode_slot, NLON)
    half = NLON // 2

    def one_sample(coeffs):
        coeff = jnp.einsum('scrl,stl->scrt', coeffs.astype(jnp.float32), masked, precision=high)
        grid = jnp.einsum('scrt,srp->tcp', coeff, waves, precision=high).astype(jnp.bfloat16)
        pre = jnp.einsum('kc,tcp->tkp', w_in.astype(jnp.float32), grid.astype(jnp.float32), precision=high)
        hidden = jax.nn.gelu(pre + b_in[None, :, None], approximate=True).astype(jnp.bfloat16)
        branch = jnp.einsum('ck,tkp->tcp', w_out.astype(jnp.float32), hidden.astype(jnp.float32), precision=high)
        mixed = (grid.astype(jnp.float32) + branch).astype(jnp.bfloat16)
        wide = mixed.astype(jnp.float32)
        rows = jnp.concatenate([jnp.roll(wide[0:1], half, axis=2), wide, jnp.roll(wide[-1:], half, axis=2)], axis=0)
        conv = jnp.zeros_like(wide)
        for i in range(3):
            band = rows[i:i + NLAT]
            for j in range(3):
                conv = conv + kernel[:, 3 * i + j][None, :, None] * jnp.roll(band, 1 - j, axis=2)
        field = wide + conv
        modes = jnp.einsum('tcp,srp->scrt', field, waves, precision=high)
        return jnp.einsum('scrt,stl->scrl', modes, masked, precision=high).astype(jnp.bfloat16)

    result = lax.map(one_sample, jnp.moveaxis(spec_in, 1, 0))
    return jnp.moveaxis(result, 0, 1)
```

```python
import functools
import math

import jax
import jax.numpy as jnp
import numpy as np
from jax import lax
from jax.experimental import pallas as pl
from jax.experimental.pallas import tpu as pltpu
from jax.sharding import PartitionSpec as P

NLON = 768
MESH = pl.DeviceIdType.MESH
F32 = jnp.float32
BF16 = jnp.bfloat16
CHUNKS = (4, 2)
GRID3 = (4, 8, 2)
NT = (((1,), (1,)), ((), ()))
TN = (((0,), (0,)), ((), ()))
NN = (((1,), (0,)), ((), ()))


def dot(a, b, dims=NN, precision=None):
    return lax.dot_general(a, b, dims, preferred_element_type=F32, precision=precision)


def far_first(k, size):
    if size == 1:
        return 0 * k
    return size // 2 + (1 - 2 * (k % 2)) * ((k + 1) // 2)


def wave_constant(modes, count):
    phase = (np.arange(modes)[:, None] * np.arange(count)[None, :]) % count
    angle = phase * (2.0 * math.pi / count)
    factor = count ** -0.5
    return np.stack([np.cos(angle) * factor, -np.sin(angle) * factor]).astype(np.float32)


def iota(shape, dim):
    return lax.broadcasted_iota(jnp.int32, shape, dim)


def body(cfg, x_ref, leg_ref, table_ref, mode_ref, mode_row, w_in, b_in, w_out, kern, out_ref,
         legv, lb, tab, wvf, wv, *rest):
    lat_n, chan_n, grid3 = cfg
    chunks = CHUNKS
    nq = len(chunks)
    slots, _, cl, _, deg = x_ref.shape
    rows = sum(chunks)
    lanes_n = slots * 2 * cl
    ltiles = lanes_n // 128
    dtiles = deg // 128
    ptiles = NLON // 128
    cr = 2 * cl
    chans = cl * chan_n
    rest = list(rest)
    take = lambda n: [rest.pop(0) for _ in range(n)]
    scr, s1, r1, lt, g, r2, mx, r3, s4, r4 = (take(nq) for _ in range(10))
    leg_sem, tab_sem, sends, recvs, locs = rest

    lat = lax.axis_index("lat")
    chan = lax.axis_index("chan")

    leg_copies = [
        [pltpu.make_async_copy(leg_ref.at[s, :, pl.ds(128 * k, 128)], legv.at[s, k], leg_sem.at[s * dtiles + k]) for k in range(dtiles)]
        for s in range(slots)
    ]
    for per in leg_copies:
        for copy in per:
            copy.start()
    tab_copy = pltpu.make_async_copy(table_ref, tab, tab_sem)
    tab_copy.start()

    barrier = pltpu.get_barrier_semaphore()

    def lat_peer(k):
        nx, nz, nc = grid3
        kz, rem = k // (nx * nc), k % (nx * nc)
        kx, kc = rem // nc, rem % nc
        dz, dx, dc = far_first(kz, nz), far_first(kx, nx), (nc - 1) - kc
        x = (lat // (nz * nc) + dx) % nx
        z = ((lat // nc) % nz + dz) % nz
        c = (lat % nc + dc) % nc
        return (x * nz + z) * nc + c

    def chan_peer(k):
        return (chan + far_first(k, chan_n)) % chan_n

    def greet_lat(k, carry):
        pl.semaphore_signal(barrier, inc=1, device_id={"lat": lat_peer(k)}, device_id_type=MESH)
        return carry

    def greet_chan(k, carry):
        pl.semaphore_signal(barrier, inc=1, device_id={"chan": chan_peer(k)}, device_id_type=MESH)
        return carry

    lax.fori_loop(0, lat_n - 1, greet_lat, 0)
    lax.fori_loop(0, chan_n - 1, greet_chan, 0)

    def start_lat(q, src, dst, at):
        def one(k, carry):
            peer = lat_peer(k)
            pltpu.make_async_remote_copy(
                src_ref=src.at[peer], dst_ref=dst.at[lat], send_sem=sends.at[at], recv_sem=recvs.at[at],
                device_id={"lat": peer}, device_id_type=MESH,
            ).start()
            return carry

        lax.fori_loop(0, lat_n - 1, one, 0)
        pltpu.make_async_copy(src.at[lat], dst.at[lat], locs.at[at]).start()

    def wait_lat(q, src, dst, at):
        pltpu.make_async_copy(src.at[lat], dst.at[lat], locs.at[at]).wait()
        pltpu.make_async_remote_copy(
            src_ref=src.at[pl.ds(0, lat_n - 1)], dst_ref=dst.at[pl.ds(0, lat_n - 1)],
            send_sem=sends.at[at], recv_sem=recvs.at[at], device_id={"lat": (lat + 1) % lat_n}, device_id_type=MESH,
        ).wait()

    lane = iota((lat_n, 128), 1)
    col_x = iota((cr, cr), 1)
    row_x = iota((cr, cr), 0)
    split = (col_x == (row_x % cl) * 2 + row_x // cl).astype(BF16)
    merge = (col_x == (row_x % 2) * cl + row_x // 2).astype(BF16)
    pair = 128 // cr
    for first in range(0, slots, pair):
        parts = []
        for s in range(first, first + pair):
            m = mode_ref[lat * slots + s]
            for copy in leg_copies[s]:
                copy.wait()
            for j in range(rows):
                for k in range(dtiles):
                    piece = legv[s, k, pl.ds(j, lat_n, stride=rows), :]
                    piece = jnp.where(lane + 128 * k >= m, piece, 0.0)
                    lb[s, j * lat_n : (j + 1) * lat_n, 128 * k : 128 * (k + 1)] = piece.astype(BF16)
            xs = dot(split, x_ref[s, 0].reshape(cr, deg)).astype(BF16)
            parts.append(dot(lb[s], xs, NT))
        both = jnp.concatenate(parts, axis=1)
        j = 0
        for q, nj in enumerate(chunks):
            for jj in range(nj):
                scr[q][first // pair, pl.ds(jj, lat_n, stride=nj), :] = both[j * lat_n : (j + 1) * lat_n]
                j += 1

    def message(q):
        nj = chunks[q]
        value = jnp.concatenate([scr[q][k] for k in range(ltiles)], axis=1)
        return value.reshape(lat_n, nj, lanes_n).astype(BF16)

    def unpack(q, received):
        nj = chunks[q]
        value = received[...].astype(F32).reshape(lat_n * nj, lanes_n)
        for k in range(ltiles):
            scr[q][k] = value[:, 128 * k : 128 * (k + 1)]
        return [
            jnp.concatenate([scr[q][k, pl.ds(jj, lat_n, stride=nj), :] for k in range(ltiles)], axis=1)
            for jj in range(nj)
        ]

    for q in range(nq):
        s1[q][...] = message(q)
    pl.semaphore_wait(barrier, lat_n - 1 + chan_n - 1)
    for q in range(nq):
        start_lat(q, s1[q], r1[q], q)

    tab_copy.wait()
    n_modes = mode_row.shape[1]
    pick = (iota((n_modes, n_modes), 0) == mode_row[...]).astype(BF16)
    for r in range(2):
        chosen = dot(pick, tab[r], TN)
        for k in range(ptiles):
            wvf[k] = chosen[:, 128 * k : 128 * (k + 1)]
        for s in range(slots):
            for k in range(ptiles):
                wv[(s * 2 + r) * lat_n : (s * 2 + r + 1) * lat_n, 128 * k : 128 * (k + 1)] = wvf[
                    k, pl.ds(s, lat_n, stride=slots), :
                ].astype(BF16)

    lane_all = iota((1, lanes_n), 1)
    mode_lane = jnp.zeros((1, lanes_n), jnp.int32)
    for s in range(slots):
        mode_lane = jnp.where(lane_all // cr == s, mode_ref[lat * slots + s], mode_lane)
    theta = mode_lane.astype(F32) * (2.0 * math.pi / NLON)
    cos_m, sin_m = jnp.cos(theta), jnp.sin(theta)
    half_turn = jnp.where(mode_lane % 2 == 0, 1.0, -1.0).astype(F32)
    spread = (iota((cl, lanes_n), 1) % cl == iota((cl, lanes_n), 0)).astype(F32)
    taps = dot(kern[...], spread, TN, precision=lax.Precision.HIGHEST)
    part_sign = jnp.where((lane_all // cl) % 2 == 0, -1.0, 1.0).astype(F32)
    direct, crossed = [], []
    for i in range(3):
        left, mid, right = (taps[3 * i + n : 3 * i + n + 1] for n in range(3))
        direct.append((left + right) * cos_m + mid + (1.0 if i == 1 else 0.0))
        crossed.append((right - left) * sin_m * part_sign)

    bias = jnp.broadcast_to(b_in[...], (128, b_in.shape[1])).T

    def slots_of(q):
        return -(-chunks[q] * ptiles // chan_n)

    def exact_chan(q):
        return chunks[q] * ptiles - (slots_of(q) - 1) * chan_n

    def chan_copies(q, src_of, dst_of, at, full_of):
        n = slots_of(q)
        even = exact_chan(q) == chan_n

        def run(act):
            for k in range(chan_n - 1):
                peer = chan_peer(k)
                count = lambda size: act(
                    pltpu.make_async_remote_copy(
                        src_ref=src_of(peer, size), dst_ref=dst_of(size), send_sem=sends.at[at],
                        recv_sem=recvs.at[at], device_id={"chan": peer}, device_id_type=MESH,
                    )
                )
                if even:
                    count(n)
                else:
                    full = full_of(peer)

                    @pl.when(full)
                    def _():
                        count(n)

                    @pl.when(jnp.logical_not(full))
                    def _():
                        count(n - 1)

        return run

    def grid_src(q):
        return lambda peer, size: g[q].at[pl.ds(peer * slots_of(q), size)]

    def start_points(q):
        at = nq + q
        extra = exact_chan(q)
        chan_copies(
            q, grid_src(q),
            lambda size: r2[q].at[pl.ds(0, size), pl.ds(pl.multiple_of(chan * cl, cl), cl)],
            at, lambda peer: peer < extra,
        )(lambda copy: copy.start())
        n = slots_of(q)

        def own(size):
            pltpu.make_async_copy(
                g[q].at[pl.ds(chan * slots_of(q), size)],
                r2[q].at[pl.ds(0, size), pl.ds(pl.multiple_of(chan * cl, cl), cl)], locs.at[at],
            ).start()

        by_size(q, own)

    def by_size(q, act):
        n, extra = slots_of(q), exact_chan(q)
        if extra == chan_n:
            act(n)
        else:

            @pl.when(chan < extra)
            def _():
                act(n)

            @pl.when(chan >= extra)
            def _():
                act(n - 1)

    def wait_points(q):
        at = nq + q

        def act(size):
            span = (chan_n - 1) * cl
            pltpu.make_async_copy(
                g[q].at[pl.ds(chan * slots_of(q), size)],
                r2[q].at[pl.ds(0, size), pl.ds(pl.multiple_of(chan * cl, cl), cl)], locs.at[at],
            ).wait()
            pltpu.make_async_remote_copy(
                src_ref=r2[q].at[pl.ds(0, size), pl.ds(0, span)], dst_ref=r2[q].at[pl.ds(0, size), pl.ds(0, span)],
                send_sem=sends.at[at], recv_sem=recvs.at[at], device_id={"chan": (chan + 1) % chan_n}, device_id_type=MESH,
            ).wait_recv()

        by_size(q, act)

    def drain_sent(q, at, buffer):
        total = chunks[q] * ptiles

        def act(size):
            part = buffer.at[pl.ds(0, total - size)]
            pltpu.make_async_remote_copy(
                src_ref=part, dst_ref=part, send_sem=sends.at[at], recv_sem=recvs.at[at],
                device_id={"chan": (chan + 1) % chan_n}, device_id_type=MESH,
            ).wait_send()

        by_size(q, act)

    def start_mixed(q):
        at = 2 * nq + q

        def act(size):
            for k in range(chan_n - 1):
                peer = chan_peer(k)
                pltpu.make_async_remote_copy(
                    src_ref=mx[q].at[pl.ds(peer * slots_of(q), size)], dst_ref=r3[q].at[pl.ds(chan * slots_of(q), size)],
                    send_sem=sends.at[at], recv_sem=recvs.at[at], device_id={"chan": peer}, device_id_type=MESH,
                ).start()
            pltpu.make_async_copy(
                mx[q].at[pl.ds(chan * slots_of(q), size)], r3[q].at[pl.ds(chan * slots_of(q), size)], locs.at[at]
            ).start()

        by_size(q, act)

    def wait_mixed(q):
        at = 2 * nq + q
        total = chunks[q] * ptiles

        def act(size):
            pltpu.make_async_copy(
                mx[q].at[pl.ds(chan * slots_of(q), size)], r3[q].at[pl.ds(chan * slots_of(q), size)], locs.at[at]
            ).wait()
            peer = {"chan": (chan + 1) % chan_n}
            sent = mx[q].at[pl.ds(0, (chan_n - 1) * size)]
            pltpu.make_async_remote_copy(
                src_ref=sent, dst_ref=sent, send_sem=sends.at[at], recv_sem=recvs.at[at], device_id=peer, device_id_type=MESH,
            ).wait_send()
            got = r3[q].at[pl.ds(0, total - size)]
            pltpu.make_async_remote_copy(
                src_ref=got, dst_ref=got, send_sem=sends.at[at], recv_sem=recvs.at[at], device_id=peer, device_id_type=MESH,
            ).wait_recv()

        by_size(q, act)

    for q, nj in enumerate(chunks):
        wait_lat(q, s1[q], r1[q], q)
        parts = unpack(q, r1[q])
        for sr in range(2 * slots):
            lt[q][sr * lat_n : (sr + 1) * lat_n, :] = jnp.concatenate(
                [part[:, cl * sr : cl * (sr + 1)] for part in parts], axis=1
            ).astype(BF16)
        grid = dot(lt[q][...], wv[...], TN).astype(BF16)
        for jj in range(nj):
            for k in range(ptiles):
                tile = jj * ptiles + k
                g[q][(tile % chan_n) * slots_of(q) + tile // chan_n] = grid[cl * jj : cl * (jj + 1), 128 * k : 128 * (k + 1)]
        start_points(q)

    for q, nj in enumerate(chunks):
        wait_points(q)
        for n in range(slots_of(q)):
            points = r2[q][n]
            pre = dot(w_in[...], points)
            hidden = jax.nn.gelu(pre + bias, approximate=True).astype(BF16)
            mixed = (points.astype(F32) + dot(w_out[...], hidden)).astype(BF16)
            for dest in range(chan_n):
                mx[q][dest * slots_of(q) + n] = mixed[cl * dest : cl * (dest + 1)]
        start_mixed(q)

    for q, nj in enumerate(chunks):
        wait_mixed(q)
        field = []
        for jj in range(nj):
            tiles = [jj * ptiles + k for k in range(ptiles)]
            field.append(jnp.concatenate([r3[q][(tile % chan_n) * slots_of(q) + tile // chan_n] for tile in tiles], axis=1))
        modes = dot(wv[...], jnp.concatenate(field, axis=0), NT)
        for jj in range(nj):
            value = jnp.concatenate(
                [modes[lat_n * sr : lat_n * (sr + 1), cl * jj : cl * (jj + 1)] for sr in range(2 * slots)], axis=1
            )
            for k in range(ltiles):
                scr[q][k, pl.ds(jj, lat_n, stride=nj), :] = value[:, 128 * k : 128 * (k + 1)]
        s4[q][...] = message(q)
        start_lat(q, s4[q], r4[q], 3 * nq + q)

    values = []
    for q in range(nq):
        wait_lat(q, s4[q], r4[q], 3 * nq + q)
        values += unpack(q, r4[q])
    row = iota((lat_n, lanes_n), 0)
    before_first = jnp.where(row == 0, half_turn * values[0], pltpu.roll(values[-1], 1, 0))
    after_last = jnp.where(row == lat_n - 1, half_turn * values[-1], pltpu.roll(values[0], lat_n - 1, 0))
    around = [before_first] + values + [after_last]
    low = (iota((lat_n, 128), 1) // cl) % 2 == 0

    def swap(a):
        pieces = []
        for k in range(ltiles):
            piece = a[:, 128 * k : 128 * (k + 1)]
            pieces.append(jnp.where(low, pltpu.roll(piece, 128 - cl, 1), pltpu.roll(piece, cl, 1)))
        return jnp.concatenate(pieces, axis=1)

    result = []
    for j in range(rows):
        straight = sum(direct[i] * around[j + i] for i in range(3))
        turned = sum(crossed[i] * swap(around[j + i]) for i in range(3))
        result.append((straight + turned).astype(BF16))
    stacked = jnp.concatenate(result, axis=0)
    for first in range(0, slots, pair):
        flipped = stacked[:, first * cr : (first + pair) * cr].T
        for s in range(first, first + pair):
            spec = dot(flipped[(s - first) * cr : (s - first + 1) * cr], lb[s]).astype(BF16)
            out_ref[s, 0] = dot(merge, spec).astype(BF16).reshape(cl, 2, deg)

    for q in range(nq):
        drain_sent(q, nq + q, g[q])


def block(cfg, table, spec_in, legendre, mode_slot, w_in, b_in, w_out, kernel):
    lat_n, chan_n, _ = cfg
    slots, batch, cl, _, deg = spec_in.shape
    rows = legendre.shape[1] // lat_n
    lanes_n = slots * 2 * cl
    n_modes = mode_slot.shape[0]
    ptiles = NLON // 128
    width = [-(-n * ptiles // chan_n) for n in CHUNKS]
    both = list(zip(CHUNKS, width))
    vm = pl.BlockSpec(memory_space=pltpu.VMEM)
    hbm = pl.BlockSpec(memory_space=pl.ANY)
    scratch = [
        pltpu.VMEM((slots, deg // 128, legendre.shape[1], 128), F32),
        pltpu.VMEM((slots, legendre.shape[1], deg), BF16),
        pltpu.VMEM((2, n_modes, NLON), BF16),
        pltpu.VMEM((ptiles, n_modes, 128), F32),
        pltpu.VMEM((2 * n_modes, NLON), BF16),
    ]
    message = lambda: [pltpu.VMEM((lat_n, n, lanes_n), BF16) for n in CHUNKS]
    scratch += [pltpu.VMEM((lanes_n // 128, lat_n * n, 128), F32) for n in CHUNKS]
    scratch += message() + message()
    scratch += [pltpu.VMEM((2 * n_modes, cl * n), BF16) for n in CHUNKS]
    scratch += [pltpu.VMEM((chan_n * t, cl, 128), BF16) for n, t in both]
    scratch += [pltpu.VMEM((t, chan_n * cl, 128), BF16) for n, t in both]
    scratch += [pltpu.VMEM((chan_n * t, cl, 128), BF16) for n, t in both]
    scratch += [pltpu.VMEM((chan_n * t, cl, 128), BF16) for n, t in both]
    scratch += message() + message()
    nq = len(CHUNKS)
    scratch += [
        pltpu.SemaphoreType.DMA((slots * deg // 128,)),
        pltpu.SemaphoreType.DMA,
        pltpu.SemaphoreType.DMA((4 * nq,)),
        pltpu.SemaphoreType.DMA((4 * nq,)),
        pltpu.SemaphoreType.DMA((4 * nq,)),
    ]
    return pl.pallas_call(
        functools.partial(body, cfg),
        out_shape=jax.ShapeDtypeStruct(spec_in.shape, BF16),
        in_specs=[vm, hbm, hbm, pl.BlockSpec(memory_space=pltpu.SMEM), vm, vm, vm, vm, vm],
        out_specs=vm,
        scratch_shapes=scratch,
        compiler_params=pltpu.CompilerParams(
            collective_id=0, has_side_effects=True, vmem_limit_bytes=60 * 1024 * 1024
        ),
        name="spherical_block",
    )(
        spec_in, legendre, jnp.asarray(table, BF16), mode_slot, mode_slot.reshape(1, -1), w_in,
        b_in.reshape(1, -1), w_out, kernel,
    )


def solution(mesh, grid3=GRID3, modes=384):
    in_specs = (
        P("lat", None, "chan", None, None),
        P("lat", None, None),
        P(),
        P(),
        P(),
        P(),
        P("chan", None),
    )
    out_specs = P("lat", None, "chan", None, None)
    cfg = (mesh.shape["lat"], mesh.shape["chan"], grid3)
    table = wave_constant(modes, NLON)
    return jax.shard_map(
        functools.partial(block, cfg, table), mesh=mesh, in_specs=in_specs, out_specs=out_specs, check_vma=False
    )
```

```python
import functools
import math

import jax
import jax.numpy as jnp
import numpy as np
from jax import lax
from jax.experimental import pallas as pl
from jax.experimental.pallas import tpu as pltpu
from jax.sharding import PartitionSpec as P

NLON = 768
MESH = pl.DeviceIdType.MESH
F32 = jnp.float32
BF16 = jnp.bfloat16
CHUNKS = (2, 2, 2)
GRID3 = (4, 8, 2)
NT = (((1,), (1,)), ((), ()))
TN = (((0,), (0,)), ((), ()))
NN = (((1,), (0,)), ((), ()))


def dot(a, b, dims=NN, precision=None):
    return lax.dot_general(a, b, dims, preferred_element_type=F32, precision=precision)


def far_first(k, size):
    if size == 1:
        return 0 * k
    return size // 2 + (1 - 2 * (k % 2)) * ((k + 1) // 2)


def wave_constant(modes, count):
    phase = (np.arange(modes)[:, None] * np.arange(count)[None, :]) % count
    angle = phase * (2.0 * math.pi / count)
    factor = count ** -0.5
    return np.stack([np.cos(angle) * factor, -np.sin(angle) * factor]).astype(np.float32)


def iota(shape, dim):
    return lax.broadcasted_iota(jnp.int32, shape, dim)


def body(cfg, x_ref, leg_ref, table_ref, mode_hbm, w_in_ref, b_ref, w_out_ref, kern_ref, out_ref,
         legv, lb, tab, wvf, wv, xv, mode_ref, mode_row, w_in, b_in, w_out, kern, *rest):
    lat_n, chan_n, grid3 = cfg
    chunks = CHUNKS
    nq = len(chunks)
    slots, _, cl, _, deg = x_ref.shape
    rows = sum(chunks)
    lanes_n = slots * 2 * cl
    ltiles = lanes_n // 128
    dtiles = deg // 128
    ptiles = NLON // 128
    cr = 2 * cl
    chans = cl * chan_n
    rest = list(rest)
    take = lambda n: [rest.pop(0) for _ in range(n)]
    scr, s1, r1, lt, g, r2, mx, r3, s4, r4 = (take(nq) for _ in range(10))
    leg_sem, in_sem, sends, recvs, locs = rest

    lat = lax.axis_index("lat")
    chan = lax.axis_index("chan")

    first_row = [lat_n * sum(chunks[:q]) for q in range(nq)]
    leg_copies = []
    for q, nj in enumerate(chunks):
        rows_q = pl.ds(first_row[q], lat_n * nj)
        leg_copies.append(
            [pltpu.make_async_copy(leg_ref.at[s, rows_q], legv.at[s, rows_q], leg_sem.at[q * slots + s]) for s in range(slots)]
        )
    in_copies = [
        pltpu.make_async_copy(src, dst, in_sem.at[k])
        for k, (src, dst) in enumerate(
            [(x_ref, xv), (mode_hbm, mode_ref), (table_ref, tab), (mode_hbm, mode_row), (w_in_ref, w_in), (b_ref, b_in), (w_out_ref, w_out), (kern_ref, kern)]
        )
    ]
    barrier = pltpu.get_barrier_semaphore()

    nx, nz, nc = grid3
    here_x, here_z, here_c = lat // (nz * nc), (lat // nc) % nz, lat % nc
    peer_x = [((here_x + far_first(k, nx)) % nx) * (nz * nc) for k in range(nx)]
    peer_c = [(here_c + nc - 1 - k) % nc for k in range(nc)]
    peer_xc = [x + c for x in peer_x for c in peer_c]
    chan_peers = [(chan + far_first(k, chan_n)) % chan_n for k in range(chan_n - 1)]

    def each_lat(act):
        def at_z(k, carry):
            z = ((here_z + far_first(k, nz)) % nz) * nc
            for base in peer_xc:
                act(base + z)
            return carry

        lax.fori_loop(0, nz - 1, at_z, 0)
        for base in peer_xc[:-1]:
            act(base + here_z * nc)

    each_lat(lambda peer: pl.semaphore_signal(barrier, inc=1, device_id={"lat": peer}, device_id_type=MESH))
    for peer in chan_peers:
        pl.semaphore_signal(barrier, inc=1, device_id={"chan": peer}, device_id_type=MESH)
    in_copies[0].start()
    in_copies[1].start()
    for copy in leg_copies[0]:
        copy.start()
    in_copies[2].start()
    for per in leg_copies[1:]:
        for copy in per:
            copy.start()
    for copy in in_copies[3:]:
        copy.start()

    def start_lat(q, src, dst, at):
        def one(peer):
            pltpu.make_async_remote_copy(
                src_ref=src.at[peer], dst_ref=dst.at[lat], send_sem=sends.at[at], recv_sem=recvs.at[at],
                device_id={"lat": peer}, device_id_type=MESH,
            ).start()

        each_lat(one)
        pltpu.make_async_copy(src.at[lat], dst.at[lat], locs.at[at]).start()

    def wait_lat(q, src, dst, at):
        pltpu.make_async_copy(src.at[lat], dst.at[lat], locs.at[at]).wait()
        pltpu.make_async_remote_copy(
            src_ref=src.at[pl.ds(0, lat_n - 1)], dst_ref=dst.at[pl.ds(0, lat_n - 1)],
            send_sem=sends.at[at], recv_sem=recvs.at[at], device_id={"lat": (lat + 1) % lat_n}, device_id_type=MESH,
        ).wait()

    col_x = iota((cr, cr), 1)
    row_x = iota((cr, cr), 0)
    split = (col_x == (row_x % cl) * 2 + row_x // cl).astype(BF16)
    merge = (col_x == (row_x % 2) * cl + row_x // 2).astype(BF16)
    pair = 128 // cr

    def message(q):
        nj = chunks[q]
        value = jnp.concatenate([scr[q][k] for k in range(ltiles)], axis=1)
        return value.reshape(lat_n, nj, lanes_n).astype(BF16)

    def unpack(q, received):
        nj = chunks[q]
        value = received[...].astype(F32).reshape(lat_n * nj, lanes_n)
        for k in range(ltiles):
            scr[q][k] = value[:, 128 * k : 128 * (k + 1)]
        return [
            jnp.concatenate([scr[q][k, pl.ds(jj, lat_n, stride=nj), :] for k in range(ltiles)], axis=1)
            for jj in range(nj)
        ]

    in_copies[0].wait()
    in_copies[1].wait()
    modes_here = [mode_ref[lat * slots + s] for s in range(slots)]
    spectra = [dot(split, xv[s, 0].reshape(cr, deg)).astype(BF16) for s in range(slots)]
    for q, nj in enumerate(chunks):
        span = slice(first_row[q], first_row[q] + lat_n * nj)
        degree = iota((lat_n * nj, deg), 1)
        for first in range(0, slots, pair):
            parts = []
            for s in range(first, first + pair):
                leg_copies[q][s].wait()
                lb[s, span] = jnp.where(degree >= modes_here[s], legv[s, span], 0.0).astype(BF16)
                parts.append(dot(lb[s, span], spectra[s], NT))
            both = jnp.concatenate(parts, axis=1)
            for jj in range(nj):
                scr[q][first // pair, pl.ds(jj, lat_n, stride=nj), :] = both[jj * lat_n : (jj + 1) * lat_n]
        s1[q][...] = message(q)
        if q == 0:
            pl.semaphore_wait(barrier, lat_n - 1 + chan_n - 1)
        start_lat(q, s1[q], r1[q], q)

    for copy in in_copies[2:]:
        copy.wait()
    n_modes = mode_row.shape[0]
    pick = (iota((n_modes, n_modes), 0) == mode_row[...].reshape(1, n_modes)).astype(BF16)
    for r in range(2):
        chosen = dot(pick, tab[r], TN)
        for k in range(ptiles):
            wvf[k] = chosen[:, 128 * k : 128 * (k + 1)]
        for s in range(slots):
            for k in range(ptiles):
                wv[(s * 2 + r) * lat_n : (s * 2 + r + 1) * lat_n, 128 * k : 128 * (k + 1)] = wvf[
                    k, pl.ds(s, lat_n, stride=slots), :
                ].astype(BF16)

    lane_all = iota((1, lanes_n), 1)
    mode_lane = jnp.zeros((1, lanes_n), jnp.int32)
    for s in range(slots):
        mode_lane = jnp.where(lane_all // cr == s, mode_ref[lat * slots + s], mode_lane)
    theta = mode_lane.astype(F32) * (2.0 * math.pi / NLON)
    cos_m, sin_m = jnp.cos(theta), jnp.sin(theta)
    half_turn = jnp.where(mode_lane % 2 == 0, 1.0, -1.0).astype(F32)
    spread = (iota((cl, lanes_n), 1) % cl == iota((cl, lanes_n), 0)).astype(F32)
    taps = dot(kern[...], spread, precision=lax.Precision.HIGHEST)
    part_sign = jnp.where((lane_all // cl) % 2 == 0, -1.0, 1.0).astype(F32)
    direct, crossed = [], []
    for i in range(3):
        left, mid, right = (taps[3 * i + n : 3 * i + n + 1] for n in range(3))
        direct.append((left + right) * cos_m + mid + (1.0 if i == 1 else 0.0))
        crossed.append((right - left) * sin_m * part_sign)

    bias = jnp.broadcast_to(b_in[...], (128, b_in.shape[1])).T

    def slots_of(q):
        return -(-chunks[q] * ptiles // chan_n)

    def exact_chan(q):
        return chunks[q] * ptiles - (slots_of(q) - 1) * chan_n

    def place(q, tile):
        n, at = tile // chan_n, tile % chan_n
        if n == slots_of(q) - 1 and 2 * exact_chan(q) == chan_n:
            at = 2 * at + q % 2
        return at, n

    def is_full(q, who):
        if 2 * exact_chan(q) == chan_n:
            return who % 2 == q % 2
        return who < exact_chan(q)

    def flat(q, tile):
        at, n = place(q, tile)
        return at * slots_of(q) + n

    def chan_copies(q, src_of, dst_of, at):
        n = slots_of(q)
        even = exact_chan(q) == chan_n

        def run(act):
            for peer in chan_peers:
                count = lambda size: act(
                    pltpu.make_async_remote_copy(
                        src_ref=src_of(peer, size), dst_ref=dst_of(size), send_sem=sends.at[at],
                        recv_sem=recvs.at[at], device_id={"chan": peer}, device_id_type=MESH,
                    )
                )
                if even:
                    count(n)
                else:
                    full = is_full(q, peer)

                    @pl.when(full)
                    def _():
                        count(n)

                    @pl.when(jnp.logical_not(full))
                    def _():
                        count(n - 1)

        return run

    def grid_src(q):
        return lambda peer, size: g[q].at[pl.ds(peer * slots_of(q), size)]

    def start_points(q):
        at = nq + q
        chan_copies(
            q, grid_src(q),
            lambda size: r2[q].at[pl.ds(0, size), pl.ds(pl.multiple_of(chan * cl, cl), cl)],
            at,
        )(lambda copy: copy.start())
        n = slots_of(q)

        def own(size):
            pltpu.make_async_copy(
                g[q].at[pl.ds(chan * slots_of(q), size)],
                r2[q].at[pl.ds(0, size), pl.ds(pl.multiple_of(chan * cl, cl), cl)], locs.at[at],
            ).start()

        by_size(q, own)

    def by_size(q, act):
        n = slots_of(q)
        if exact_chan(q) == chan_n:
            act(n)
        else:

            @pl.when(is_full(q, chan))
            def _():
                act(n)

            @pl.when(jnp.logical_not(is_full(q, chan)))
            def _():
                act(n - 1)

    def wait_points(q):
        at = nq + q

        def act(size):
            span = (chan_n - 1) * cl
            pltpu.make_async_copy(
                g[q].at[pl.ds(chan * slots_of(q), size)],
                r2[q].at[pl.ds(0, size), pl.ds(pl.multiple_of(chan * cl, cl), cl)], locs.at[at],
            ).wait()
            pltpu.make_async_remote_copy(
                src_ref=r2[q].at[pl.ds(0, size), pl.ds(0, span)], dst_ref=r2[q].at[pl.ds(0, size), pl.ds(0, span)],
                send_sem=sends.at[at], recv_sem=recvs.at[at], device_id={"chan": (chan + 1) % chan_n}, device_id_type=MESH,
            ).wait_recv()

        by_size(q, act)

    def drain_sent(q, at, buffer):
        total = chunks[q] * ptiles

        def act(size):
            part = buffer.at[pl.ds(0, total - size)]
            pltpu.make_async_remote_copy(
                src_ref=part, dst_ref=part, send_sem=sends.at[at], recv_sem=recvs.at[at],
                device_id={"chan": (chan + 1) % chan_n}, device_id_type=MESH,
            ).wait_send()

        by_size(q, act)

    def start_mixed(q):
        at = 2 * nq + q

        def act(size):
            for peer in chan_peers:
                pltpu.make_async_remote_copy(
                    src_ref=mx[q].at[pl.ds(peer * slots_of(q), size)], dst_ref=r3[q].at[pl.ds(chan * slots_of(q), size)],
                    send_sem=sends.at[at], recv_sem=recvs.at[at], device_id={"chan": peer}, device_id_type=MESH,
                ).start()
            pltpu.make_async_copy(
                mx[q].at[pl.ds(chan * slots_of(q), size)], r3[q].at[pl.ds(chan * slots_of(q), size)], locs.at[at]
            ).start()

        by_size(q, act)

    def wait_mixed(q):
        at = 2 * nq + q
        total = chunks[q] * ptiles

        def act(size):
            pltpu.make_async_copy(
                mx[q].at[pl.ds(chan * slots_of(q), size)], r3[q].at[pl.ds(chan * slots_of(q), size)], locs.at[at]
            ).wait()
            peer = {"chan": (chan + 1) % chan_n}
            sent = mx[q].at[pl.ds(0, (chan_n - 1) * size)]
            pltpu.make_async_remote_copy(
                src_ref=sent, dst_ref=sent, send_sem=sends.at[at], recv_sem=recvs.at[at], device_id=peer, device_id_type=MESH,
            ).wait_send()
            got = r3[q].at[pl.ds(0, total - size)]
            pltpu.make_async_remote_copy(
                src_ref=got, dst_ref=got, send_sem=sends.at[at], recv_sem=recvs.at[at], device_id=peer, device_id_type=MESH,
            ).wait_recv()

        by_size(q, act)

    for q, nj in enumerate(chunks):
        wait_lat(q, s1[q], r1[q], q)
        parts = unpack(q, r1[q])
        for sr in range(2 * slots):
            lt[q][sr * lat_n : (sr + 1) * lat_n, :] = jnp.concatenate(
                [part[:, cl * sr : cl * (sr + 1)] for part in parts], axis=1
            ).astype(BF16)
        grid = dot(lt[q][...], wv[...], TN).astype(BF16)
        for jj in range(nj):
            for k in range(ptiles):
                tile = jj * ptiles + k
                g[q][flat(q, tile)] = grid[cl * jj : cl * (jj + 1), 128 * k : 128 * (k + 1)]
        start_points(q)

    for q, nj in enumerate(chunks):
        wait_points(q)
        for n in range(slots_of(q)):
            points = r2[q][n]
            pre = dot(w_in[...], points)
            hidden = jax.nn.gelu(pre + bias, approximate=True).astype(BF16)
            mixed = (points.astype(F32) + dot(w_out[...], hidden)).astype(BF16)
            for dest in range(chan_n):
                mx[q][dest * slots_of(q) + n] = mixed[cl * dest : cl * (dest + 1)]
        start_mixed(q)

    for q, nj in enumerate(chunks):
        wait_mixed(q)
        field = []
        for jj in range(nj):
            tiles = [jj * ptiles + k for k in range(ptiles)]
            field.append(jnp.concatenate([r3[q][flat(q, tile)] for tile in tiles], axis=1))
        modes = dot(jnp.concatenate(field, axis=0), wv[...], NT).T
        for jj in range(nj):
            value = jnp.concatenate(
                [modes[lat_n * sr : lat_n * (sr + 1), cl * jj : cl * (jj + 1)] for sr in range(2 * slots)], axis=1
            )
            for k in range(ltiles):
                scr[q][k, pl.ds(jj, lat_n, stride=nj), :] = value[:, 128 * k : 128 * (k + 1)]
        s4[q][...] = message(q)
        start_lat(q, s4[q], r4[q], 3 * nq + q)

    values = []
    for q in range(nq):
        wait_lat(q, s4[q], r4[q], 3 * nq + q)
        values += unpack(q, r4[q])
    n_rows = lat_n * rows
    row = iota((n_rows, 1), 0)
    here = jnp.concatenate(values, axis=0)
    before = jnp.where(row == 0, half_turn * here, pltpu.roll(here, 1, 0))
    after = jnp.where(row == n_rows - 1, half_turn * here, pltpu.roll(here, n_rows - 1, 0))
    low = (iota((n_rows, 128), 1) // cl) % 2 == 0

    def swap(a):
        pieces = []
        for k in range(ltiles):
            piece = a[:, 128 * k : 128 * (k + 1)]
            pieces.append(jnp.where(low, pltpu.roll(piece, 128 - cl, 1), pltpu.roll(piece, cl, 1)))
        return jnp.concatenate(pieces, axis=1)

    straight = direct[0] * before + direct[1] * here + direct[2] * after
    turned = crossed[0] * swap(before) + crossed[1] * swap(here) + crossed[2] * swap(after)
    stacked = (straight + turned).astype(BF16)
    for first in range(0, slots, pair):
        flipped = stacked[:, first * cr : (first + pair) * cr].T
        for s in range(first, first + pair):
            spec = dot(flipped[(s - first) * cr : (s - first + 1) * cr], lb[s]).astype(BF16)
            out_ref[s] = dot(merge, spec).astype(BF16)

    for q in range(nq):
        drain_sent(q, nq + q, g[q])


def block(cfg, table, spec_in, legendre, mode_slot, w_in, b_in, w_out, kernel):
    lat_n, chan_n, _ = cfg
    slots, batch, cl, _, deg = spec_in.shape
    rows = legendre.shape[1] // lat_n
    lanes_n = slots * 2 * cl
    n_modes = mode_slot.shape[0]
    ptiles = NLON // 128
    width = [-(-n * ptiles // chan_n) for n in CHUNKS]
    both = list(zip(CHUNKS, width))
    vm = pl.BlockSpec(memory_space=pltpu.VMEM)
    hbm = pl.BlockSpec(memory_space=pltpu.HBM)
    scratch = [
        pltpu.VMEM(legendre.shape, F32),
        pltpu.VMEM((slots, legendre.shape[1], deg), BF16),
        pltpu.VMEM((2, n_modes, NLON), BF16),
        pltpu.VMEM((ptiles, n_modes, 128), F32),
        pltpu.VMEM((2 * n_modes, NLON), BF16),
        pltpu.VMEM(spec_in.shape, BF16),
        pltpu.SMEM(mode_slot.shape, jnp.int32),
        pltpu.VMEM(mode_slot.shape, jnp.int32),
        pltpu.VMEM(w_in.shape, BF16),
        pltpu.VMEM((1, b_in.shape[0]), F32),
        pltpu.VMEM(w_out.shape, BF16),
        pltpu.VMEM(kernel.shape[::-1], F32),
    ]
    message = lambda: [pltpu.VMEM((lat_n, n, lanes_n), BF16) for n in CHUNKS]
    scratch += [pltpu.VMEM((lanes_n // 128, lat_n * n, 128), F32) for n in CHUNKS]
    scratch += message() + message()
    scratch += [pltpu.VMEM((2 * n_modes, cl * n), BF16) for n in CHUNKS]
    scratch += [pltpu.VMEM((chan_n * t, cl, 128), BF16) for n, t in both]
    scratch += [pltpu.VMEM((t, chan_n * cl, 128), BF16) for n, t in both]
    scratch += [pltpu.VMEM((chan_n * t, cl, 128), BF16) for n, t in both]
    scratch += [pltpu.VMEM((chan_n * t, cl, 128), BF16) for n, t in both]
    scratch += message() + message()
    nq = len(CHUNKS)
    scratch += [
        pltpu.SemaphoreType.DMA((slots * nq,)),
        pltpu.SemaphoreType.DMA((8,)),
        pltpu.SemaphoreType.DMA((4 * nq,)),
        pltpu.SemaphoreType.DMA((4 * nq,)),
        pltpu.SemaphoreType.DMA((4 * nq,)),
    ]
    return pl.pallas_call(
        functools.partial(body, cfg),
        out_shape=jax.ShapeDtypeStruct((slots, 2 * cl, deg), BF16),
        in_specs=[hbm] * 8,
        out_specs=vm,
        scratch_shapes=scratch,
        compiler_params=pltpu.CompilerParams(
            collective_id=0, has_side_effects=True, vmem_limit_bytes=60 * 1024 * 1024
        ),
        name="spherical_block",
    )(
        spec_in, legendre, jnp.asarray(table, BF16), mode_slot, w_in,
        b_in.reshape(1, -1), w_out, kernel.T,
    ).reshape(spec_in.shape)


def solution(mesh, grid3=GRID3, modes=384):
    in_specs = (
        P("lat", None, "chan", None, None),
        P("lat", None, None),
        P(),
        P(),
        P(),
        P(),
        P("chan", None),
    )
    out_specs = P("lat", None, "chan", None, None)
    cfg = (mesh.shape["lat"], mesh.shape["chan"], grid3)
    table = wave_constant(modes, NLON)
    return jax.shard_map(
        functools.partial(block, cfg, table), mesh=mesh, in_specs=in_specs, out_specs=out_specs, check_vma=False
    )
```

```python
import functools
import math

import jax
import jax.numpy as jnp
import numpy as np
from jax import lax
from jax.experimental import pallas as pl
from jax.experimental.pallas import tpu as pltpu
from jax.sharding import PartitionSpec as P

NLON = 768
MESH = pl.DeviceIdType.MESH
F32 = jnp.float32
BF16 = jnp.bfloat16
CHUNKS = (2, 2, 2)
GRID3 = (4, 8, 2)
NT = (((1,), (1,)), ((), ()))
TN = (((0,), (0,)), ((), ()))
NN = (((1,), (0,)), ((), ()))


def dot(a, b, dims=NN, precision=None):
    return lax.dot_general(a, b, dims, preferred_element_type=F32, precision=precision)


def far_first(k, size):
    if size == 1:
        return 0 * k
    return size // 2 + (1 - 2 * (k % 2)) * ((k + 1) // 2)


def wave_constant(modes, count):
    phase = (np.arange(modes)[:, None] * np.arange(count)[None, :]) % count
    angle = phase * (2.0 * math.pi / count)
    factor = count ** -0.5
    return np.stack([np.cos(angle) * factor, -np.sin(angle) * factor]).astype(np.float32)


def iota(shape, dim):
    return lax.broadcasted_iota(jnp.int32, shape, dim)


def body(cfg, x_ref, leg_ref, table_ref, mode_hbm, w_in_ref, b_ref, w_out_ref, kern_ref, out_ref,
         legv, lb, tab, wvf, wv, wvt, acc, xv, mode_ref, mode_row, w_in, b_in, w_out, kern, *rest):
    lat_n, chan_n, grid3 = cfg
    chunks = CHUNKS
    nq = len(chunks)
    slots, _, cl, _, deg = x_ref.shape
    rows = sum(chunks)
    lanes_n = slots * 2 * cl
    ltiles = lanes_n // 128
    dtiles = deg // 128
    ptiles = NLON // 128
    cr = 2 * cl
    chans = cl * chan_n
    rest = list(rest)
    take = lambda n: [rest.pop(0) for _ in range(n)]
    scr, s1, r1, lt, g, r2, mx, r3, s4, r4 = (take(nq) for _ in range(10))
    leg_sem, in_sem, sends, recvs, locs = rest

    lat = lax.axis_index("lat")
    chan = lax.axis_index("chan")

    first_row = [lat_n * sum(chunks[:q]) for q in range(nq)]
    leg_copies = []
    for q, nj in enumerate(chunks):
        rows_q = pl.ds(first_row[q], lat_n * nj)
        leg_copies.append(
            [pltpu.make_async_copy(leg_ref.at[s, rows_q], legv.at[s, rows_q], leg_sem.at[q * slots + s]) for s in range(slots)]
        )
    in_copies = [
        pltpu.make_async_copy(src, dst, in_sem.at[k])
        for k, (src, dst) in enumerate(
            [(x_ref, xv), (mode_hbm, mode_ref), (table_ref, tab), (mode_hbm, mode_row), (w_in_ref, w_in), (b_ref, b_in), (w_out_ref, w_out), (kern_ref, kern)]
        )
    ]
    barrier = pltpu.get_barrier_semaphore()

    nx, nz, nc = grid3
    here_x, here_z, here_c = lat // (nz * nc), (lat // nc) % nz, lat % nc
    peer_x = [((here_x + far_first(k, nx)) % nx) * (nz * nc) for k in range(nx)]
    peer_c = [(here_c + nc - 1 - k) % nc for k in range(nc)]
    peer_xc = [x + c for x in peer_x for c in peer_c]
    chan_peers = [(chan + far_first(k, chan_n)) % chan_n for k in range(chan_n - 1)]

    def each_lat(act):
        def at_z(k, carry):
            z = ((here_z + far_first(k, nz)) % nz) * nc
            for base in peer_xc:
                act(base + z)
            return carry

        lax.fori_loop(0, nz - 1, at_z, 0)
        for base in peer_xc[:-1]:
            act(base + here_z * nc)

    in_copies[0].start()
    in_copies[1].start()
    for copy in leg_copies[0]:
        copy.start()

    each_lat(lambda peer: pl.semaphore_signal(barrier, inc=1, device_id={"lat": peer}, device_id_type=MESH))
    for peer in chan_peers:
        pl.semaphore_signal(barrier, inc=1, device_id={"chan": peer}, device_id_type=MESH)
    in_copies[2].start()
    for per in leg_copies[1:]:
        for copy in per:
            copy.start()
    for copy in in_copies[3:]:
        copy.start()

    def start_lat(q, src, dst, at):
        def one(peer):
            pltpu.make_async_remote_copy(
                src_ref=src.at[peer], dst_ref=dst.at[lat], send_sem=sends.at[at], recv_sem=recvs.at[at],
                device_id={"lat": peer}, device_id_type=MESH,
            ).start()

        each_lat(one)
        pltpu.make_async_copy(src.at[lat], dst.at[lat], locs.at[at]).start()

    def wait_lat(q, src, dst, at):
        pltpu.make_async_copy(src.at[lat], dst.at[lat], locs.at[at]).wait()
        pltpu.make_async_remote_copy(
            src_ref=src.at[pl.ds(0, lat_n - 1)], dst_ref=dst.at[pl.ds(0, lat_n - 1)],
            send_sem=sends.at[at], recv_sem=recvs.at[at], device_id={"lat": (lat + 1) % lat_n}, device_id_type=MESH,
        ).wait()

    col_x = iota((cr, cr), 1)
    row_x = iota((cr, cr), 0)
    split = (col_x == (row_x % cl) * 2 + row_x // cl).astype(BF16)
    pair = 128 // cr
    wide_col, wide_row = iota((128, 128), 1), iota((128, 128), 0)
    merge = (wide_col == wide_row // cr * cr + (wide_row % 2) * cl + wide_row % cr // 2).astype(BF16)

    def message(q):
        nj = chunks[q]
        value = jnp.concatenate([scr[q][k] for k in range(ltiles)], axis=1)
        return value.reshape(lat_n, nj, lanes_n).astype(BF16)

    def unpack(q, received):
        nj = chunks[q]
        value = received[...].astype(F32).reshape(lat_n * nj, lanes_n)
        for k in range(ltiles):
            scr[q][k] = value[:, 128 * k : 128 * (k + 1)]
        return [
            jnp.concatenate([scr[q][k, pl.ds(jj, lat_n, stride=nj), :] for k in range(ltiles)], axis=1)
            for jj in range(nj)
        ]

    in_copies[0].wait()
    in_copies[1].wait()
    modes_here = [mode_ref[lat * slots + s] for s in range(slots)]
    spectra = [dot(split, xv[s, 0].reshape(cr, deg)).astype(BF16) for s in range(slots)]
    for q, nj in enumerate(chunks):
        span = slice(first_row[q], first_row[q] + lat_n * nj)
        degree = iota((lat_n * nj, deg), 1)
        for copy in leg_copies[q]:
            copy.wait()
        masked = [jnp.where(degree >= modes_here[s], legv[s, span], 0.0).astype(BF16) for s in range(slots)]
        products = [dot(masked[s], spectra[s], NT) for s in range(slots)]
        for s in range(slots):
            lb[s, span] = masked[s]
        for first in range(0, slots, pair):
            both = jnp.concatenate(products[first : first + pair], axis=1)
            for jj in range(nj):
                scr[q][first // pair, pl.ds(jj, lat_n, stride=nj), :] = both[jj * lat_n : (jj + 1) * lat_n]
        s1[q][...] = message(q)
    pl.semaphore_wait(barrier, lat_n - 1 + chan_n - 1)
    for q in range(nq):
        start_lat(q, s1[q], r1[q], q)

    for copy in in_copies[2:]:
        copy.wait()
    n_modes = mode_row.shape[0]
    pick = (iota((n_modes, n_modes), 0) == mode_row[...].reshape(1, n_modes)).astype(BF16)
    for r in range(2):
        chosen = dot(pick, tab[r], TN)
        for k in range(ptiles):
            wvf[k] = chosen[:, 128 * k : 128 * (k + 1)]
        for s in range(slots):
            for k in range(ptiles):
                wv[(s * 2 + r) * lat_n : (s * 2 + r + 1) * lat_n, 128 * k : 128 * (k + 1)] = wvf[
                    k, pl.ds(s, lat_n, stride=slots), :
                ].astype(BF16)

    lane_all = iota((1, lanes_n), 1)
    mode_lane = jnp.zeros((1, lanes_n), jnp.int32)
    for s in range(slots):
        mode_lane = jnp.where(lane_all // cr == s, mode_ref[lat * slots + s], mode_lane)
    theta = mode_lane.astype(F32) * (2.0 * math.pi / NLON)
    cos_m, sin_m = jnp.cos(theta), jnp.sin(theta)
    half_turn = jnp.where(mode_lane % 2 == 0, 1.0, -1.0).astype(F32)
    spread = (iota((cl, lanes_n), 1) % cl == iota((cl, lanes_n), 0)).astype(F32)
    taps = dot(kern[...], spread, precision=lax.Precision.HIGHEST)
    part_sign = jnp.where((lane_all // cl) % 2 == 0, -1.0, 1.0).astype(F32)
    direct, crossed = [], []
    for i in range(3):
        left, mid, right = (taps[3 * i + n : 3 * i + n + 1] for n in range(3))
        direct.append((left + right) * cos_m + mid + (1.0 if i == 1 else 0.0))
        crossed.append((right - left) * sin_m * part_sign)

    bias = jnp.broadcast_to(b_in[...], (128, b_in.shape[1])).T

    def slots_of(q):
        return -(-chunks[q] * ptiles // chan_n)

    def exact_chan(q):
        return chunks[q] * ptiles - (slots_of(q) - 1) * chan_n

    def place(q, tile):
        n, at = tile // chan_n, tile % chan_n
        if n == slots_of(q) - 1 and 2 * exact_chan(q) == chan_n:
            at = 2 * at + q % 2
        return at, n

    def is_full(q, who):
        if 2 * exact_chan(q) == chan_n:
            return who % 2 == q % 2
        return who < exact_chan(q)

    def flat(q, tile):
        at, n = place(q, tile)
        return at * slots_of(q) + n

    def chan_copies(q, src_of, dst_of, at):
        n = slots_of(q)
        even = exact_chan(q) == chan_n

        def run(act):
            for peer in chan_peers:
                count = lambda size: act(
                    pltpu.make_async_remote_copy(
                        src_ref=src_of(peer, size), dst_ref=dst_of(size), send_sem=sends.at[at],
                        recv_sem=recvs.at[at], device_id={"chan": peer}, device_id_type=MESH,
                    )
                )
                if even:
                    count(n)
                else:
                    full = is_full(q, peer)

                    @pl.when(full)
                    def _():
                        count(n)

                    @pl.when(jnp.logical_not(full))
                    def _():
                        count(n - 1)

        return run

    def grid_src(q):
        return lambda peer, size: g[q].at[pl.ds(peer * slots_of(q), size)]

    def start_points(q):
        at = nq + q
        chan_copies(
            q, grid_src(q),
            lambda size: r2[q].at[pl.ds(0, size), pl.ds(pl.multiple_of(chan * cl, cl), cl)],
            at,
        )(lambda copy: copy.start())
        n = slots_of(q)

        def own(size):
            pltpu.make_async_copy(
                g[q].at[pl.ds(chan * slots_of(q), size)],
                r2[q].at[pl.ds(0, size), pl.ds(pl.multiple_of(chan * cl, cl), cl)], locs.at[at],
            ).start()

        by_size(q, own)

    def by_size(q, act):
        n = slots_of(q)
        if exact_chan(q) == chan_n:
            act(n)
        else:

            @pl.when(is_full(q, chan))
            def _():
                act(n)

            @pl.when(jnp.logical_not(is_full(q, chan)))
            def _():
                act(n - 1)

    def wait_points(q):
        at = nq + q

        def act(size):
            span = (chan_n - 1) * cl
            pltpu.make_async_copy(
                g[q].at[pl.ds(chan * slots_of(q), size)],
                r2[q].at[pl.ds(0, size), pl.ds(pl.multiple_of(chan * cl, cl), cl)], locs.at[at],
            ).wait()
            pltpu.make_async_remote_copy(
                src_ref=r2[q].at[pl.ds(0, size), pl.ds(0, span)], dst_ref=r2[q].at[pl.ds(0, size), pl.ds(0, span)],
                send_sem=sends.at[at], recv_sem=recvs.at[at], device_id={"chan": (chan + 1) % chan_n}, device_id_type=MESH,
            ).wait_recv()

        by_size(q, act)

    def drain_sent(q, at, buffer):
        total = chunks[q] * ptiles

        def act(size):
            part = buffer.at[pl.ds(0, total - size)]
            pltpu.make_async_remote_copy(
                src_ref=part, dst_ref=part, send_sem=sends.at[at], recv_sem=recvs.at[at],
                device_id={"chan": (chan + 1) % chan_n}, device_id_type=MESH,
            ).wait_send()

        by_size(q, act)

    def start_mixed(q):
        at = 2 * nq + q

        def act(size):
            for peer in chan_peers:
                pltpu.make_async_remote_copy(
                    src_ref=mx[q].at[pl.ds(peer * slots_of(q), size)], dst_ref=r3[q].at[pl.ds(chan * slots_of(q), size)],
                    send_sem=sends.at[at], recv_sem=recvs.at[at], device_id={"chan": peer}, device_id_type=MESH,
                ).start()
            pltpu.make_async_copy(
                mx[q].at[pl.ds(chan * slots_of(q), size)], r3[q].at[pl.ds(chan * slots_of(q), size)], locs.at[at]
            ).start()

        by_size(q, act)

    def wait_mixed(q):
        at = 2 * nq + q
        total = chunks[q] * ptiles

        def act(size):
            pltpu.make_async_copy(
                mx[q].at[pl.ds(chan * slots_of(q), size)], r3[q].at[pl.ds(chan * slots_of(q), size)], locs.at[at]
            ).wait()
            peer = {"chan": (chan + 1) % chan_n}
            sent = mx[q].at[pl.ds(0, (chan_n - 1) * size)]
            pltpu.make_async_remote_copy(
                src_ref=sent, dst_ref=sent, send_sem=sends.at[at], recv_sem=recvs.at[at], device_id=peer, device_id_type=MESH,
            ).wait_send()
            got = r3[q].at[pl.ds(0, total - size)]
            pltpu.make_async_remote_copy(
                src_ref=got, dst_ref=got, send_sem=sends.at[at], recv_sem=recvs.at[at], device_id=peer, device_id_type=MESH,
            ).wait_recv()

        by_size(q, act)

    for q, nj in enumerate(chunks):
        wait_lat(q, s1[q], r1[q], q)
        parts = unpack(q, r1[q])
        for sr in range(2 * slots):
            lt[q][sr * lat_n : (sr + 1) * lat_n, :] = jnp.concatenate(
                [part[:, cl * sr : cl * (sr + 1)] for part in parts], axis=1
            ).astype(BF16)
        grid = dot(lt[q][...], wv[...], TN).astype(BF16)
        for jj in range(nj):
            for k in range(ptiles):
                tile = jj * ptiles + k
                g[q][flat(q, tile)] = grid[cl * jj : cl * (jj + 1), 128 * k : 128 * (k + 1)]
        start_points(q)

    for q, nj in enumerate(chunks):
        wait_points(q)
        for n in range(0, slots_of(q), 2):
            tiles = range(n, min(n + 2, slots_of(q)))
            points = jnp.concatenate([r2[q][tile] for tile in tiles], axis=1)
            pre = dot(w_in[...], points)
            hidden = jax.nn.gelu(pre + jnp.concatenate([bias for _ in tiles], axis=1), approximate=True).astype(BF16)
            mixed = (points.astype(F32) + dot(w_out[...], hidden)).astype(BF16)
            for dest in range(chan_n):
                for k, tile in enumerate(tiles):
                    mx[q][dest * slots_of(q) + tile] = mixed[cl * dest : cl * (dest + 1), 128 * k : 128 * (k + 1)]
        start_mixed(q)

    wvt[...] = wv[...].T

    for q, nj in enumerate(chunks):
        wait_mixed(q)
        field = []
        for jj in range(nj):
            tiles = [jj * ptiles + k for k in range(ptiles)]
            field.append(jnp.concatenate([r3[q][flat(q, tile)] for tile in tiles], axis=1))
        modes = dot(jnp.concatenate(field, axis=0), wvt[...]).T
        for jj in range(nj):
            value = jnp.concatenate(
                [modes[lat_n * sr : lat_n * (sr + 1), cl * jj : cl * (jj + 1)] for sr in range(2 * slots)], axis=1
            )
            for k in range(ltiles):
                scr[q][k, pl.ds(jj, lat_n, stride=nj), :] = value[:, 128 * k : 128 * (k + 1)]
        s4[q][...] = message(q)
        start_lat(q, s4[q], r4[q], 3 * nq + q)

    def swap(a):
        low = (iota((a.shape[0], 128), 1) // cl) % 2 == 0
        pieces = []
        for k in range(ltiles):
            piece = a[:, 128 * k : 128 * (k + 1)]
            pieces.append(jnp.where(low, pltpu.roll(piece, 128 - cl, 1), pltpu.roll(piece, cl, 1)))
        return jnp.concatenate(pieces, axis=1)

    edge = min(16, lat_n * chunks[0])
    carried = None
    for q, nj in enumerate(chunks):
        wait_lat(q, s4[q], r4[q], 3 * nq + q)
        here = jnp.concatenate(unpack(q, r4[q]), axis=0)
        turned = swap(here)
        to_next, own, to_last = (direct[i] * here + crossed[i] * turned for i in range(3))
        n_rows = lat_n * nj
        row = iota((n_rows, 1), 0)
        from_last = half_turn * to_next[:1] if q == 0 else carried
        from_next = half_turn * to_last[n_rows - 1 :] if q == nq - 1 else jnp.zeros_like(from_last)
        carried = to_next[n_rows - 1 :]
        field = own + jnp.where(row == 0, from_last, pltpu.roll(to_next, 1, 0))
        field = field + jnp.where(row == n_rows - 1, from_next, pltpu.roll(to_last, n_rows - 1, 0))
        field = field.astype(BF16)
        start = first_row[q]
        if q > 0:
            missing = jnp.where(iota((edge, lanes_n), 0) == edge - 1, to_last[:1], 0.0).astype(BF16)
            field = jnp.concatenate([missing, field], axis=0)
            start -= edge
        span = slice(start, first_row[q] + n_rows)
        for first in range(0, slots, pair):
            left = dot(merge, field[:, first * cr : (first + pair) * cr], NT).astype(BF16)
            for s in range(first, first + pair):
                part = dot(left[(s - first) * cr : (s - first + 1) * cr], lb[s, span])
                if q > 0:
                    part = part + acc[s]
                if q < nq - 1:
                    acc[s] = part
                else:
                    out_ref[s, 0] = part.astype(BF16).reshape(cl, 2, deg)

    for q in range(nq):
        drain_sent(q, nq + q, g[q])


def block(cfg, table, spec_in, legendre, mode_slot, w_in, b_in, w_out, kernel):
    lat_n, chan_n, _ = cfg
    slots, batch, cl, _, deg = spec_in.shape
    rows = legendre.shape[1] // lat_n
    lanes_n = slots * 2 * cl
    n_modes = mode_slot.shape[0]
    ptiles = NLON // 128
    width = [-(-n * ptiles // chan_n) for n in CHUNKS]
    both = list(zip(CHUNKS, width))
    vm = pl.BlockSpec(memory_space=pltpu.VMEM)
    hbm = pl.BlockSpec(memory_space=pltpu.HBM)
    scratch = [
        pltpu.VMEM(legendre.shape, F32),
        pltpu.VMEM((slots, legendre.shape[1], deg), BF16),
        pltpu.VMEM((2, n_modes, NLON), BF16),
        pltpu.VMEM((ptiles, n_modes, 128), F32),
        pltpu.VMEM((2 * n_modes, NLON), BF16),
        pltpu.VMEM((NLON, 2 * n_modes), BF16),
        pltpu.VMEM((slots, 2 * cl, deg), F32),
        pltpu.VMEM(spec_in.shape, BF16),
        pltpu.SMEM(mode_slot.shape, jnp.int32),
        pltpu.VMEM(mode_slot.shape, jnp.int32),
        pltpu.VMEM(w_in.shape, BF16),
        pltpu.VMEM((1, b_in.shape[0]), F32),
        pltpu.VMEM(w_out.shape, BF16),
        pltpu.VMEM(kernel.shape[::-1], F32),
    ]
    message = lambda: [pltpu.VMEM((lat_n, n, lanes_n), BF16) for n in CHUNKS]
    scratch += [pltpu.VMEM((lanes_n // 128, lat_n * n, 128), F32) for n in CHUNKS]
    scratch += message() + message()
    scratch += [pltpu.VMEM((2 * n_modes, cl * n), BF16) for n in CHUNKS]
    scratch += [pltpu.VMEM((chan_n * t, cl, 128), BF16) for n, t in both]
    scratch += [pltpu.VMEM((t, chan_n * cl, 128), BF16) for n, t in both]
    scratch += [pltpu.VMEM((chan_n * t, cl, 128), BF16) for n, t in both]
    scratch += [pltpu.VMEM((chan_n * t, cl, 128), BF16) for n, t in both]
    scratch += message() + message()
    nq = len(CHUNKS)
    scratch += [
        pltpu.SemaphoreType.DMA((slots * nq,)),
        pltpu.SemaphoreType.DMA((8,)),
        pltpu.SemaphoreType.DMA((4 * nq,)),
        pltpu.SemaphoreType.DMA((4 * nq,)),
        pltpu.SemaphoreType.DMA((4 * nq,)),
    ]
    return pl.pallas_call(
        functools.partial(body, cfg),
        out_shape=pltpu.VMEM(spec_in.shape, BF16),
        in_specs=[hbm] * 8,
        out_specs=vm,
        scratch_shapes=scratch,
        compiler_params=pltpu.CompilerParams(
            collective_id=0, has_side_effects=True, vmem_limit_bytes=60 * 1024 * 1024
        ),
        name="spherical_block",
    )(
        spec_in, legendre, jnp.asarray(table, BF16), mode_slot, w_in,
        b_in.reshape(1, -1), w_out, kernel.T,
    )


def solution(mesh, grid3=GRID3, modes=384):
    in_specs = (
        P("lat", None, "chan", None, None),
        P("lat", None, None),
        P(),
        P(),
        P(),
        P(),
        P("chan", None),
    )
    out_specs = P("lat", None, "chan", None, None)
    cfg = (mesh.shape["lat"], mesh.shape["chan"], grid3)
    table = wave_constant(modes, NLON)
    return jax.shard_map(
        functools.partial(block, cfg, table), mesh=mesh, in_specs=in_specs, out_specs=out_specs, check_vma=False
    )
```

```python
import functools
import math

import jax
import jax.numpy as jnp
import numpy as np
from jax import lax
from jax.experimental import pallas as pl
from jax.experimental.pallas import tpu as pltpu
from jax.sharding import PartitionSpec as P

NLON = 768
MESH = pl.DeviceIdType.MESH
F32 = jnp.float32
BF16 = jnp.bfloat16
CHUNKS = (2, 2, 2)
GRID3 = (4, 8, 2)
NT = (((1,), (1,)), ((), ()))
TN = (((0,), (0,)), ((), ()))
NN = (((1,), (0,)), ((), ()))


def dot(a, b, dims=NN, precision=None):
    return lax.dot_general(a, b, dims, preferred_element_type=F32, precision=precision)


def far_first(k, size):
    if size == 1:
        return 0 * k
    return size // 2 + (1 - 2 * (k % 2)) * ((k + 1) // 2)


def wave_constant(modes, count):
    phase = (np.arange(modes)[:, None] * np.arange(count)[None, :]) % count
    angle = phase * (2.0 * math.pi / count)
    factor = count ** -0.5
    return np.stack([np.cos(angle) * factor, -np.sin(angle) * factor]).astype(np.float32)


def iota(shape, dim):
    return lax.broadcasted_iota(jnp.int32, shape, dim)


def body(cfg, x_ref, leg_ref, table_ref, mode_hbm, w_in_ref, b_ref, w_out_ref, kern_ref, out_ref,
         legv, lb, tab, wvf, wv, wvt, acc, xv, mode_ref, mode_row, w_in, b_in, w_out, kern, *rest):
    lat_n, chan_n, grid3 = cfg
    chunks = CHUNKS
    nq = len(chunks)
    slots, _, cl, _, deg = x_ref.shape
    rows = sum(chunks)
    lanes_n = slots * 2 * cl
    ltiles = lanes_n // 128
    dtiles = deg // 128
    ptiles = NLON // 128
    cr = 2 * cl
    chans = cl * chan_n
    rest = list(rest)
    take = lambda n: [rest.pop(0) for _ in range(n)]
    scr, s1, r1, lt, g, r2, mx, r3, s4, r4 = (take(nq) for _ in range(10))
    in_sem, sends, recvs, locs = rest

    lat = lax.axis_index("lat")
    chan = lax.axis_index("chan")

    first_row = [lat_n * sum(chunks[:q]) for q in range(nq)]
    leg_copies = []
    for q, nj in enumerate(chunks):
        rows_q = pl.ds(first_row[q], lat_n * nj)
        leg_copies.append(
            [pltpu.make_async_copy(leg_ref.at[s, rows_q], legv.at[s, rows_q], locs.at[q]) for s in range(slots)]
        )
    in_copies = [
        pltpu.make_async_copy(src, dst, in_sem.at[k] if k < 5 else sends.at[nq + k - 5])
        for k, (src, dst) in enumerate(
            [(x_ref, xv), (mode_hbm, mode_ref), (table_ref, tab), (mode_hbm, mode_row), (w_in_ref, w_in), (b_ref, b_in), (w_out_ref, w_out), (kern_ref, kern)]
        )
    ]
    barrier = pltpu.get_barrier_semaphore()

    nx, nz, nc = grid3
    here_x, here_z, here_c = lat // (nz * nc), (lat // nc) % nz, lat % nc
    peer_x = [((here_x + far_first(k, nx)) % nx) * (nz * nc) for k in range(nx)]
    peer_c = [(here_c + nc - 1 - k) % nc for k in range(nc)]
    peer_xc = [x + c for x in peer_x for c in peer_c]
    chan_peers = [(chan + far_first(k, chan_n)) % chan_n for k in range(chan_n - 1)]

    def each_lat(act):
        def at_z(k, carry):
            z = ((here_z + far_first(k, nz)) % nz) * nc
            for base in peer_xc:
                act(base + z)
            return carry

        lax.fori_loop(0, nz - 1, at_z, 0)
        for base in peer_xc[:-1]:
            act(base + here_z * nc)

    in_copies[0].start()
    in_copies[1].start()
    for copy in leg_copies[0]:
        copy.start()

    each_lat(lambda peer: pl.semaphore_signal(barrier, inc=1, device_id={"lat": peer}, device_id_type=MESH))
    for peer in chan_peers:
        pl.semaphore_signal(barrier, inc=1, device_id={"chan": peer}, device_id_type=MESH)
    in_copies[2].start()
    for per in leg_copies[1:]:
        for copy in per:
            copy.start()
    for copy in in_copies[3:]:
        copy.start()

    def sent_sem(at):
        return sends.at[at % nq if at // nq in (0, 3) else nq + at % nq]

    def start_lat(q, src, dst, at):
        def one(peer):
            pltpu.make_async_remote_copy(
                src_ref=src.at[peer], dst_ref=dst.at[lat], send_sem=sent_sem(at), recv_sem=recvs.at[at],
                device_id={"lat": peer}, device_id_type=MESH,
            ).start()

        each_lat(one)
        pltpu.make_async_copy(src.at[lat], dst.at[lat], locs.at[at % nq]).start()

    def wait_lat(q, src, dst, at):
        pltpu.make_async_copy(src.at[lat], dst.at[lat], locs.at[at % nq]).wait()
        pltpu.make_async_remote_copy(
            src_ref=src.at[pl.ds(0, lat_n - 1)], dst_ref=dst.at[pl.ds(0, lat_n - 1)],
            send_sem=sent_sem(at), recv_sem=recvs.at[at], device_id={"lat": (lat + 1) % lat_n}, device_id_type=MESH,
        ).wait()

    col_x = iota((cr, cr), 1)
    row_x = iota((cr, cr), 0)
    split = (col_x == (row_x % cl) * 2 + row_x // cl).astype(BF16)
    pair = 128 // cr
    wide_col, wide_row = iota((128, 128), 1), iota((128, 128), 0)
    merge = (wide_col == wide_row // cr * cr + (wide_row % 2) * cl + wide_row % cr // 2).astype(BF16)

    def message(q):
        nj = chunks[q]
        value = jnp.concatenate([scr[q][k] for k in range(ltiles)], axis=1)
        return value.reshape(lat_n, nj, lanes_n).astype(BF16)

    def unpack(q, received):
        nj = chunks[q]
        value = received[...].astype(F32).reshape(lat_n * nj, lanes_n)
        for k in range(ltiles):
            scr[q][k] = value[:, 128 * k : 128 * (k + 1)]
        return [
            jnp.concatenate([scr[q][k, pl.ds(jj, lat_n, stride=nj), :] for k in range(ltiles)], axis=1)
            for jj in range(nj)
        ]

    in_copies[0].wait()
    in_copies[1].wait()
    modes_here = [mode_ref[lat * slots + s] for s in range(slots)]
    spectra = [dot(split, xv[s, 0].reshape(cr, deg)).astype(BF16) for s in range(slots)]
    for q, nj in enumerate(chunks):
        span = slice(first_row[q], first_row[q] + lat_n * nj)
        degree = iota((lat_n * nj, deg), 1)
        rows_q = pl.ds(first_row[q], lat_n * nj)
        pltpu.make_async_copy(leg_ref.at[:, rows_q], legv.at[:, rows_q], locs.at[q]).wait()
        masked = [jnp.where(degree >= modes_here[s], legv[s, span], 0.0).astype(BF16) for s in range(slots)]
        products = [dot(masked[s], spectra[s], NT) for s in range(slots)]
        for s in range(slots):
            lb[s, span] = masked[s]
        for first in range(0, slots, pair):
            both = jnp.concatenate(products[first : first + pair], axis=1)
            for jj in range(nj):
                scr[q][first // pair, pl.ds(jj, lat_n, stride=nj), :] = both[jj * lat_n : (jj + 1) * lat_n]
        s1[q][...] = message(q)
    pl.semaphore_wait(barrier, lat_n - 1 + chan_n - 1)
    for q in range(nq):
        start_lat(q, s1[q], r1[q], q)

    for copy in in_copies[2:]:
        copy.wait()
    n_modes = mode_row.shape[0]
    pick = (iota((n_modes, n_modes), 0) == mode_row[...].reshape(1, n_modes)).astype(BF16)
    for r in range(2):
        chosen = dot(pick, tab[r], TN)
        for k in range(ptiles):
            wvf[k] = chosen[:, 128 * k : 128 * (k + 1)]
        for s in range(slots):
            for k in range(ptiles):
                wv[(s * 2 + r) * lat_n : (s * 2 + r + 1) * lat_n, 128 * k : 128 * (k + 1)] = wvf[
                    k, pl.ds(s, lat_n, stride=slots), :
                ].astype(BF16)

    lane_all = iota((1, lanes_n), 1)
    mode_lane = jnp.zeros((1, lanes_n), jnp.int32)
    for s in range(slots):
        mode_lane = jnp.where(lane_all // cr == s, mode_ref[lat * slots + s], mode_lane)
    theta = mode_lane.astype(F32) * (2.0 * math.pi / NLON)
    cos_m, sin_m = jnp.cos(theta), jnp.sin(theta)
    half_turn = jnp.where(mode_lane % 2 == 0, 1.0, -1.0).astype(F32)
    spread = (iota((cl, lanes_n), 1) % cl == iota((cl, lanes_n), 0)).astype(F32)
    taps = dot(kern[...], spread, precision=lax.Precision.HIGHEST)
    part_sign = jnp.where((lane_all // cl) % 2 == 0, -1.0, 1.0).astype(F32)
    direct, crossed = [], []
    for i in range(3):
        left, mid, right = (taps[3 * i + n : 3 * i + n + 1] for n in range(3))
        direct.append((left + right) * cos_m + mid + (1.0 if i == 1 else 0.0))
        crossed.append((right - left) * sin_m * part_sign)

    bias = jnp.broadcast_to(b_in[...], (128, b_in.shape[1])).T

    def slots_of(q):
        return -(-chunks[q] * ptiles // chan_n)

    def exact_chan(q):
        return chunks[q] * ptiles - (slots_of(q) - 1) * chan_n

    def place(q, tile):
        n, at = tile // chan_n, tile % chan_n
        if n == slots_of(q) - 1 and 2 * exact_chan(q) == chan_n:
            at = 2 * at + q % 2
        return at, n

    def is_full(q, who):
        if 2 * exact_chan(q) == chan_n:
            return who % 2 == q % 2
        return who < exact_chan(q)

    def flat(q, tile):
        at, n = place(q, tile)
        return at * slots_of(q) + n

    def chan_copies(q, src_of, dst_of, at):
        n = slots_of(q)
        even = exact_chan(q) == chan_n

        def run(act):
            for peer in chan_peers:
                count = lambda size: act(
                    pltpu.make_async_remote_copy(
                        src_ref=src_of(peer, size), dst_ref=dst_of(size), send_sem=sent_sem(at),
                        recv_sem=recvs.at[at], device_id={"chan": peer}, device_id_type=MESH,
                    )
                )
                if even:
                    count(n)
                else:
                    full = is_full(q, peer)

                    @pl.when(full)
                    def _():
                        count(n)

                    @pl.when(jnp.logical_not(full))
                    def _():
                        count(n - 1)

        return run

    def grid_src(q):
        return lambda peer, size: g[q].at[pl.ds(peer * slots_of(q), size)]

    def start_points(q):
        at = nq + q
        chan_copies(
            q, grid_src(q),
            lambda size: r2[q].at[pl.ds(0, size), pl.ds(pl.multiple_of(chan * cl, cl), cl)],
            at,
        )(lambda copy: copy.start())
        n = slots_of(q)

        def own(size):
            pltpu.make_async_copy(
                g[q].at[pl.ds(chan * slots_of(q), size)],
                r2[q].at[pl.ds(0, size), pl.ds(pl.multiple_of(chan * cl, cl), cl)], locs.at[at % nq],
            ).start()

        by_size(q, own)

    def by_size(q, act):
        n = slots_of(q)
        if exact_chan(q) == chan_n:
            act(n)
        else:

            @pl.when(is_full(q, chan))
            def _():
                act(n)

            @pl.when(jnp.logical_not(is_full(q, chan)))
            def _():
                act(n - 1)

    def wait_points(q):
        at = nq + q

        def act(size):
            span = (chan_n - 1) * cl
            pltpu.make_async_copy(
                g[q].at[pl.ds(chan * slots_of(q), size)],
                r2[q].at[pl.ds(0, size), pl.ds(pl.multiple_of(chan * cl, cl), cl)], locs.at[at % nq],
            ).wait()
            pltpu.make_async_remote_copy(
                src_ref=r2[q].at[pl.ds(0, size), pl.ds(0, span)], dst_ref=r2[q].at[pl.ds(0, size), pl.ds(0, span)],
                send_sem=sent_sem(at), recv_sem=recvs.at[at], device_id={"chan": (chan + 1) % chan_n}, device_id_type=MESH,
            ).wait_recv()

        by_size(q, act)

    def drain_sent(q, at, buffer):
        total = chunks[q] * ptiles

        def act(size):
            part = buffer.at[pl.ds(0, total - size)]
            pltpu.make_async_remote_copy(
                src_ref=part, dst_ref=part, send_sem=sent_sem(at), recv_sem=recvs.at[at],
                device_id={"chan": (chan + 1) % chan_n}, device_id_type=MESH,
            ).wait_send()

        by_size(q, act)

    def start_mixed(q):
        at = 2 * nq + q

        def act(size):
            for peer in chan_peers:
                pltpu.make_async_remote_copy(
                    src_ref=mx[q].at[pl.ds(peer * slots_of(q), size)], dst_ref=r3[q].at[pl.ds(chan * slots_of(q), size)],
                    send_sem=sent_sem(at), recv_sem=recvs.at[at], device_id={"chan": peer}, device_id_type=MESH,
                ).start()
            pltpu.make_async_copy(
                mx[q].at[pl.ds(chan * slots_of(q), size)], r3[q].at[pl.ds(chan * slots_of(q), size)], locs.at[at % nq]
            ).start()

        by_size(q, act)

    def wait_mixed(q):
        at = 2 * nq + q
        total = chunks[q] * ptiles

        def act(size):
            pltpu.make_async_copy(
                mx[q].at[pl.ds(chan * slots_of(q), size)], r3[q].at[pl.ds(chan * slots_of(q), size)], locs.at[at % nq]
            ).wait()
            peer = {"chan": (chan + 1) % chan_n}
            sent = mx[q].at[pl.ds(0, (chan_n - 1) * size)]
            pltpu.make_async_remote_copy(
                src_ref=sent, dst_ref=sent, send_sem=sent_sem(at), recv_sem=recvs.at[at], device_id=peer, device_id_type=MESH,
            ).wait_send()
            got = r3[q].at[pl.ds(0, total - size)]
            pltpu.make_async_remote_copy(
                src_ref=got, dst_ref=got, send_sem=sent_sem(at), recv_sem=recvs.at[at], device_id=peer, device_id_type=MESH,
            ).wait_recv()

        by_size(q, act)

    for q, nj in enumerate(chunks):
        wait_lat(q, s1[q], r1[q], q)
        parts = [part.astype(BF16) for part in unpack(q, r1[q])]
        for sr in range(2 * slots):
            lt[q][sr * lat_n : (sr + 1) * lat_n, :] = jnp.concatenate(
                [part[:, cl * sr : cl * (sr + 1)] for part in parts], axis=1
            )
        grid = dot(lt[q][...], wv[...], TN).astype(BF16)
        for jj in range(nj):
            for k in range(ptiles):
                tile = jj * ptiles + k
                g[q][flat(q, tile)] = grid[cl * jj : cl * (jj + 1), 128 * k : 128 * (k + 1)]
        start_points(q)

    for q, nj in enumerate(chunks):
        wait_points(q)
        drain_sent(q, nq + q, g[q])
        for n in range(0, slots_of(q), 2):
            tiles = range(n, min(n + 2, slots_of(q)))
            points = jnp.concatenate([r2[q][tile] for tile in tiles], axis=1)
            pre = dot(w_in[...], points)
            hidden = jax.nn.gelu(pre + jnp.concatenate([bias for _ in tiles], axis=1), approximate=True).astype(BF16)
            mixed = (points.astype(F32) + dot(w_out[...], hidden)).astype(BF16)
            for dest in range(chan_n):
                for k, tile in enumerate(tiles):
                    mx[q][dest * slots_of(q) + tile] = mixed[cl * dest : cl * (dest + 1), 128 * k : 128 * (k + 1)]
        start_mixed(q)

    wvt[...] = wv[...].T

    for q, nj in enumerate(chunks):
        wait_mixed(q)
        field = []
        for jj in range(nj):
            tiles = [jj * ptiles + k for k in range(ptiles)]
            field.append(jnp.concatenate([r3[q][flat(q, tile)] for tile in tiles], axis=1))
        modes = dot(jnp.concatenate(field, axis=0), wvt[...]).T
        for jj in range(nj):
            value = jnp.concatenate(
                [modes[lat_n * sr : lat_n * (sr + 1), cl * jj : cl * (jj + 1)] for sr in range(2 * slots)], axis=1
            )
            for k in range(ltiles):
                scr[q][k, pl.ds(jj, lat_n, stride=nj), :] = value[:, 128 * k : 128 * (k + 1)]
        s4[q][...] = message(q)
        start_lat(q, s4[q], r4[q], 3 * nq + q)

    def swap(a):
        low = (iota((a.shape[0], 128), 1) // cl) % 2 == 0
        pieces = []
        for k in range(ltiles):
            piece = a[:, 128 * k : 128 * (k + 1)]
            pieces.append(jnp.where(low, pltpu.roll(piece, 128 - cl, 1), pltpu.roll(piece, cl, 1)))
        return jnp.concatenate(pieces, axis=1)

    edge = min(16, lat_n * chunks[0])
    carried = None
    for q, nj in enumerate(chunks):
        wait_lat(q, s4[q], r4[q], 3 * nq + q)
        here = jnp.concatenate(unpack(q, r4[q]), axis=0)
        turned = swap(here)
        to_next, own, to_last = (direct[i] * here + crossed[i] * turned for i in range(3))
        n_rows = lat_n * nj
        row = iota((n_rows, 1), 0)
        from_last = half_turn * to_next[:1] if q == 0 else carried
        from_next = half_turn * to_last[n_rows - 1 :] if q == nq - 1 else jnp.zeros_like(from_last)
        carried = to_next[n_rows - 1 :]
        field = own + jnp.where(row == 0, from_last, pltpu.roll(to_next, 1, 0))
        field = field + jnp.where(row == n_rows - 1, from_next, pltpu.roll(to_last, n_rows - 1, 0))
        field = field.astype(BF16)
        start = first_row[q]
        if q > 0:
            missing = jnp.where(iota((edge, lanes_n), 0) == edge - 1, to_last[:1], 0.0).astype(BF16)
            field = jnp.concatenate([missing, field], axis=0)
            start -= edge
        span = slice(start, first_row[q] + n_rows)
        left = [
            dot(merge, field[:, first * cr : (first + pair) * cr], NT).astype(BF16) for first in range(0, slots, pair)
        ]
        products = [
            dot(left[s // pair][s % pair * cr : (s % pair + 1) * cr], lb[s, span]) for s in range(slots)
        ]
        for s in range(slots):
            part = products[s] if q == 0 else products[s] + acc[s]
            if q < nq - 1:
                acc[s] = part
            else:
                out_ref[s, 0] = part.astype(BF16).reshape(cl, 2, deg)


def block(cfg, table, spec_in, legendre, mode_slot, w_in, b_in, w_out, kernel):
    lat_n, chan_n, _ = cfg
    slots, batch, cl, _, deg = spec_in.shape
    rows = legendre.shape[1] // lat_n
    lanes_n = slots * 2 * cl
    n_modes = mode_slot.shape[0]
    ptiles = NLON // 128
    width = [-(-n * ptiles // chan_n) for n in CHUNKS]
    both = list(zip(CHUNKS, width))
    vm = pl.BlockSpec(memory_space=pltpu.VMEM)
    hbm = pl.BlockSpec(memory_space=pltpu.HBM)
    scratch = [
        pltpu.VMEM(legendre.shape, F32),
        pltpu.VMEM((slots, legendre.shape[1], deg), BF16),
        pltpu.VMEM((2, n_modes, NLON), BF16),
        pltpu.VMEM((ptiles, n_modes, 128), F32),
        pltpu.VMEM((2 * n_modes, NLON), BF16),
        pltpu.VMEM((NLON, 2 * n_modes), BF16),
        pltpu.VMEM((slots, 2 * cl, deg), F32),
        pltpu.VMEM(spec_in.shape, BF16),
        pltpu.SMEM(mode_slot.shape, jnp.int32),
        pltpu.VMEM(mode_slot.shape, jnp.int32),
        pltpu.VMEM(w_in.shape, BF16),
        pltpu.VMEM((1, b_in.shape[0]), F32),
        pltpu.VMEM(w_out.shape, BF16),
        pltpu.VMEM(kernel.shape[::-1], F32),
    ]
    message = lambda: [pltpu.VMEM((lat_n, n, lanes_n), BF16) for n in CHUNKS]
    scratch += [pltpu.VMEM((lanes_n // 128, lat_n * n, 128), F32) for n in CHUNKS]
    scratch += message() + message()
    scratch += [pltpu.VMEM((2 * n_modes, cl * n), BF16) for n in CHUNKS]
    scratch += [pltpu.VMEM((chan_n * t, cl, 128), BF16) for n, t in both]
    scratch += [pltpu.VMEM((t, chan_n * cl, 128), BF16) for n, t in both]
    scratch += [pltpu.VMEM((chan_n * t, cl, 128), BF16) for n, t in both]
    scratch += [pltpu.VMEM((chan_n * t, cl, 128), BF16) for n, t in both]
    scratch += message() + message()
    nq = len(CHUNKS)
    scratch += [
        pltpu.SemaphoreType.DMA((5,)),
        pltpu.SemaphoreType.DMA((2 * nq,)),
        pltpu.SemaphoreType.DMA((4 * nq,)),
        pltpu.SemaphoreType.DMA((nq,)),
    ]
    return pl.pallas_call(
        functools.partial(body, cfg),
        out_shape=pltpu.VMEM(spec_in.shape, BF16),
        in_specs=[hbm] * 8,
        out_specs=vm,
        scratch_shapes=scratch,
        compiler_params=pltpu.CompilerParams(
            collective_id=0, has_side_effects=True, vmem_limit_bytes=60 * 1024 * 1024
        ),
        name="spherical_block",
    )(
        spec_in, legendre, jnp.asarray(table, BF16), mode_slot, w_in,
        b_in.reshape(1, -1), w_out, kernel.T,
    )


def solution(mesh, grid3=GRID3, modes=384):
    in_specs = (
        P("lat", None, "chan", None, None),
        P("lat", None, None),
        P(),
        P(),
        P(),
        P(),
        P("chan", None),
    )
    out_specs = P("lat", None, "chan", None, None)
    cfg = (mesh.shape["lat"], mesh.shape["chan"], grid3)
    table = wave_constant(modes, NLON)
    return jax.shard_map(
        functools.partial(block, cfg, table), mesh=mesh, in_specs=in_specs, out_specs=out_specs, check_vma=False
    )
```

```python
import functools
import math

import jax
import jax.numpy as jnp
import numpy as np
from jax import lax
from jax.experimental import pallas as pl
from jax.experimental.pallas import tpu as pltpu
from jax.sharding import PartitionSpec as P

NLON = 768
MESH = pl.DeviceIdType.MESH
F32 = jnp.float32
BF16 = jnp.bfloat16
CHUNKS = (2, 2, 2)
GRID3 = (4, 8, 2)
NT = (((1,), (1,)), ((), ()))
TN = (((0,), (0,)), ((), ()))
NN = (((1,), (0,)), ((), ()))


def dot(a, b, dims=NN, precision=None):
    return lax.dot_general(a, b, dims, preferred_element_type=F32, precision=precision)


def gelu(x):
    a = math.sqrt(2.0 / math.pi)
    half = 0.5 * x
    return half + half * jnp.tanh(x * (a + (a * 0.044715) * (x * x)))


def far_first(k, size):
    if size == 1:
        return 0 * k
    return size // 2 + (1 - 2 * (k % 2)) * ((k + 1) // 2)


def wave_constant(modes, count):
    phase = (np.arange(modes)[:, None] * np.arange(count)[None, :]) % count
    angle = phase * (2.0 * math.pi / count)
    factor = count ** -0.5
    return np.stack([np.cos(angle) * factor, -np.sin(angle) * factor]).astype(np.float32)


def iota(shape, dim):
    return lax.broadcasted_iota(jnp.int32, shape, dim)


def body(cfg, x_ref, leg_ref, table_ref, mode_hbm, w_in_ref, b_ref, w_out_ref, kern_ref, out_ref,
         legv, lb, tab, wvf, wv, wvt, acc, xv, mode_ref, mode_row, w_in, b_in, w_out, kern, *rest):
    lat_n, chan_n, grid3 = cfg
    chunks = CHUNKS
    nq = len(chunks)
    slots, _, cl, _, deg = x_ref.shape
    rows = sum(chunks)
    lanes_n = slots * 2 * cl
    ltiles = lanes_n // 128
    dtiles = deg // 128
    ptiles = NLON // 128
    cr = 2 * cl
    chans = cl * chan_n
    rest = list(rest)
    take = lambda n: [rest.pop(0) for _ in range(n)]
    scr, s1, r1, lt, g, r2, mx, r3, s4, r4 = (take(nq) for _ in range(10))
    in_sem, sends, recvs, locs = rest

    lat = lax.axis_index("lat")
    chan = lax.axis_index("chan")

    first_row = [lat_n * sum(chunks[:q]) for q in range(nq)]
    leg_copies = []
    for q, nj in enumerate(chunks):
        rows_q = pl.ds(first_row[q], lat_n * nj)
        leg_copies.append(
            [pltpu.make_async_copy(leg_ref.at[s, rows_q], legv.at[s, rows_q], locs.at[q]) for s in range(slots)]
        )
    in_copies = [
        pltpu.make_async_copy(src, dst, in_sem.at[k] if k < 5 else sends.at[nq + k - 5])
        for k, (src, dst) in enumerate(
            [(x_ref, xv), (mode_hbm, mode_ref), (table_ref, tab), (mode_hbm, mode_row), (w_in_ref, w_in), (b_ref, b_in), (w_out_ref, w_out), (kern_ref, kern)]
        )
    ]
    barrier = pltpu.get_barrier_semaphore()

    nx, nz, nc = grid3
    here_x, here_z, here_c = lat // (nz * nc), (lat // nc) % nz, lat % nc
    peer_x = [((here_x + far_first(k, nx)) % nx) * (nz * nc) for k in range(nx)]
    peer_c = [(here_c + nc - 1 - k) % nc for k in range(nc)]
    peer_xc = [x + c for x in peer_x for c in peer_c]
    chan_peers = [(chan + far_first(k, chan_n)) % chan_n for k in range(chan_n - 1)]

    def each_lat(act):
        def at_z(k, carry):
            z = ((here_z + far_first(k, nz)) % nz) * nc
            for base in peer_xc:
                act(base + z)
            return carry

        lax.fori_loop(0, nz - 1, at_z, 0)
        for base in peer_xc[:-1]:
            act(base + here_z * nc)

    in_copies[0].start()
    in_copies[1].start()
    for copy in leg_copies[0]:
        copy.start()

    each_lat(lambda peer: pl.semaphore_signal(barrier, inc=1, device_id={"lat": peer}, device_id_type=MESH))
    for peer in chan_peers:
        pl.semaphore_signal(barrier, inc=1, device_id={"chan": peer}, device_id_type=MESH)
    in_copies[2].start()
    for per in leg_copies[1:]:
        for copy in per:
            copy.start()
    for copy in in_copies[3:]:
        copy.start()

    def sent_sem(at):
        return sends.at[at % nq if at // nq in (0, 3) else nq + at % nq]

    def start_lat(q, src, dst, at):
        def one(peer):
            pltpu.make_async_remote_copy(
                src_ref=src.at[peer], dst_ref=dst.at[lat], send_sem=sent_sem(at), recv_sem=recvs.at[at],
                device_id={"lat": peer}, device_id_type=MESH,
            ).start()

        each_lat(one)
        pltpu.make_async_copy(src.at[lat], dst.at[lat], locs.at[at % nq]).start()

    def wait_lat(q, src, dst, at):
        pltpu.make_async_copy(src.at[lat], dst.at[lat], locs.at[at % nq]).wait()
        pltpu.make_async_remote_copy(
            src_ref=src.at[pl.ds(0, lat_n - 1)], dst_ref=dst.at[pl.ds(0, lat_n - 1)],
            send_sem=sent_sem(at), recv_sem=recvs.at[at], device_id={"lat": (lat + 1) % lat_n}, device_id_type=MESH,
        ).wait()

    col_x = iota((cr, cr), 1)
    row_x = iota((cr, cr), 0)
    split = (col_x == (row_x % cl) * 2 + row_x // cl).astype(BF16)
    pair = 128 // cr
    wide_col, wide_row = iota((128, 128), 1), iota((128, 128), 0)
    merge = (wide_col == wide_row // cr * cr + (wide_row % 2) * cl + wide_row % cr // 2).astype(BF16)

    def message(q):
        nj = chunks[q]
        value = jnp.concatenate([scr[q][k] for k in range(ltiles)], axis=1)
        return value.reshape(lat_n, nj, lanes_n).astype(BF16)

    def unpack(q, received):
        nj = chunks[q]
        value = received[...].astype(F32).reshape(lat_n * nj, lanes_n)
        for k in range(ltiles):
            scr[q][k] = value[:, 128 * k : 128 * (k + 1)]
        return [
            jnp.concatenate([scr[q][k, pl.ds(jj, lat_n, stride=nj), :] for k in range(ltiles)], axis=1)
            for jj in range(nj)
        ]

    in_copies[0].wait()
    in_copies[1].wait()
    modes_here = [mode_ref[lat * slots + s] for s in range(slots)]
    spectra = [dot(split, xv[s, 0].reshape(cr, deg)).astype(BF16) for s in range(slots)]
    for q, nj in enumerate(chunks):
        span = slice(first_row[q], first_row[q] + lat_n * nj)
        degree = iota((lat_n * nj, deg), 1)
        rows_q = pl.ds(first_row[q], lat_n * nj)
        pltpu.make_async_copy(leg_ref.at[:, rows_q], legv.at[:, rows_q], locs.at[q]).wait()
        masked = [jnp.where(degree >= modes_here[s], legv[s, span], 0.0).astype(BF16) for s in range(slots)]
        products = [dot(masked[s], spectra[s], NT) for s in range(slots)]
        for s in range(slots):
            lb[s, span] = masked[s]
        for first in range(0, slots, pair):
            both = jnp.concatenate(products[first : first + pair], axis=1)
            for jj in range(nj):
                scr[q][first // pair, pl.ds(jj, lat_n, stride=nj), :] = both[jj * lat_n : (jj + 1) * lat_n]
        s1[q][...] = message(q)
    pl.semaphore_wait(barrier, lat_n - 1 + chan_n - 1)
    for q in range(nq):
        start_lat(q, s1[q], r1[q], q)

    for copy in in_copies[2:]:
        copy.wait()
    n_modes = mode_row.shape[0]
    pick = (iota((n_modes, n_modes), 0) == mode_row[...].reshape(1, n_modes)).astype(BF16)
    for r in range(2):
        chosen = dot(pick, tab[r], TN)
        for k in range(ptiles):
            wvf[k] = chosen[:, 128 * k : 128 * (k + 1)]
        for s in range(slots):
            for k in range(ptiles):
                wv[(s * 2 + r) * lat_n : (s * 2 + r + 1) * lat_n, 128 * k : 128 * (k + 1)] = wvf[
                    k, pl.ds(s, lat_n, stride=slots), :
                ].astype(BF16)

    lane_all = iota((1, lanes_n), 1)
    mode_lane = jnp.zeros((1, lanes_n), jnp.int32)
    for s in range(slots):
        mode_lane = jnp.where(lane_all // cr == s, mode_ref[lat * slots + s], mode_lane)
    theta = mode_lane.astype(F32) * (2.0 * math.pi / NLON)
    cos_m, sin_m = jnp.cos(theta), jnp.sin(theta)
    half_turn = jnp.where(mode_lane % 2 == 0, 1.0, -1.0).astype(F32)
    spread = (iota((cl, lanes_n), 1) % cl == iota((cl, lanes_n), 0)).astype(F32)
    taps = dot(kern[...], spread, precision=lax.Precision.HIGHEST)
    part_sign = jnp.where((lane_all // cl) % 2 == 0, -1.0, 1.0).astype(F32)
    direct, crossed = [], []
    for i in range(3):
        left, mid, right = (taps[3 * i + n : 3 * i + n + 1] for n in range(3))
        direct.append((left + right) * cos_m + mid + (1.0 if i == 1 else 0.0))
        crossed.append((right - left) * sin_m * part_sign)

    bias = jnp.broadcast_to(b_in[...], (128, b_in.shape[1])).T

    def slots_of(q):
        return -(-chunks[q] * ptiles // chan_n)

    def exact_chan(q):
        return chunks[q] * ptiles - (slots_of(q) - 1) * chan_n

    def first_columns(q):
        nj = chunks[q]
        even = slots_of(q) == 2 and chan_n % nj == 0 and chan_n // nj < ptiles
        return chan_n // nj if even else ptiles

    def place(q, tile):
        head = first_columns(q)
        if head < ptiles:
            jj, k = tile // ptiles, tile % ptiles
            n, at = (0, jj * head + k) if k < head else (1, jj * (ptiles - head) + k - head)
        else:
            n, at = tile // chan_n, tile % chan_n
        if n == slots_of(q) - 1 and 2 * exact_chan(q) == chan_n:
            at = 2 * at + q % 2
        return at, n

    def is_full(q, who):
        if 2 * exact_chan(q) == chan_n:
            return who % 2 == q % 2
        return who < exact_chan(q)

    def flat(q, tile):
        at, n = place(q, tile)
        return at * slots_of(q) + n

    def start_points(q, n):
        at = nq + q
        columns = pl.ds(pl.multiple_of(chan * cl, cl), cl)

        def send(peer):
            pltpu.make_async_remote_copy(
                src_ref=g[q].at[peer * slots_of(q) + n], dst_ref=r2[q].at[n, columns], send_sem=sent_sem(at),
                recv_sem=recvs.at[at], device_id={"chan": peer}, device_id_type=MESH,
            ).start()

        for peer in chan_peers:
            if n < slots_of(q) - 1 or exact_chan(q) == chan_n:
                send(peer)
            else:
                pl.when(is_full(q, peer))(functools.partial(send, peer))

    def start_own(q):
        def own(size):
            pltpu.make_async_copy(
                g[q].at[pl.ds(chan * slots_of(q), size)],
                r2[q].at[pl.ds(0, size), pl.ds(pl.multiple_of(chan * cl, cl), cl)], locs.at[q],
            ).start()

        by_size(q, own)

    def by_size(q, act):
        n = slots_of(q)
        if exact_chan(q) == chan_n:
            act(n)
        else:

            @pl.when(is_full(q, chan))
            def _():
                act(n)

            @pl.when(jnp.logical_not(is_full(q, chan)))
            def _():
                act(n - 1)

    def wait_points(q):
        at = nq + q

        def act(size):
            span = (chan_n - 1) * cl
            pltpu.make_async_copy(
                g[q].at[pl.ds(chan * slots_of(q), size)],
                r2[q].at[pl.ds(0, size), pl.ds(pl.multiple_of(chan * cl, cl), cl)], locs.at[at % nq],
            ).wait()
            pltpu.make_async_remote_copy(
                src_ref=r2[q].at[pl.ds(0, size), pl.ds(0, span)], dst_ref=r2[q].at[pl.ds(0, size), pl.ds(0, span)],
                send_sem=sent_sem(at), recv_sem=recvs.at[at], device_id={"chan": (chan + 1) % chan_n}, device_id_type=MESH,
            ).wait_recv()

        by_size(q, act)

    def drain_sent(q, at, buffer):
        total = chunks[q] * ptiles

        def act(size):
            part = buffer.at[pl.ds(0, total - size)]
            pltpu.make_async_remote_copy(
                src_ref=part, dst_ref=part, send_sem=sent_sem(at), recv_sem=recvs.at[at],
                device_id={"chan": (chan + 1) % chan_n}, device_id_type=MESH,
            ).wait_send()

        by_size(q, act)

    def start_mixed(q):
        at = 2 * nq + q

        def act(size):
            for peer in chan_peers:
                pltpu.make_async_remote_copy(
                    src_ref=mx[q].at[pl.ds(peer * slots_of(q), size)], dst_ref=r3[q].at[pl.ds(chan * slots_of(q), size)],
                    send_sem=sent_sem(at), recv_sem=recvs.at[at], device_id={"chan": peer}, device_id_type=MESH,
                ).start()
            pltpu.make_async_copy(
                mx[q].at[pl.ds(chan * slots_of(q), size)], r3[q].at[pl.ds(chan * slots_of(q), size)], locs.at[at % nq]
            ).start()

        by_size(q, act)

    def wait_mixed(q):
        at = 2 * nq + q
        total = chunks[q] * ptiles

        def act(size):
            pltpu.make_async_copy(
                mx[q].at[pl.ds(chan * slots_of(q), size)], r3[q].at[pl.ds(chan * slots_of(q), size)], locs.at[at % nq]
            ).wait()
            peer = {"chan": (chan + 1) % chan_n}
            sent = mx[q].at[pl.ds(0, (chan_n - 1) * size)]
            pltpu.make_async_remote_copy(
                src_ref=sent, dst_ref=sent, send_sem=sent_sem(at), recv_sem=recvs.at[at], device_id=peer, device_id_type=MESH,
            ).wait_send()
            got = r3[q].at[pl.ds(0, total - size)]
            pltpu.make_async_remote_copy(
                src_ref=got, dst_ref=got, send_sem=sent_sem(at), recv_sem=recvs.at[at], device_id=peer, device_id_type=MESH,
            ).wait_recv()

        by_size(q, act)

    for q, nj in enumerate(chunks):
        wait_lat(q, s1[q], r1[q], q)
        parts = [part.astype(BF16) for part in unpack(q, r1[q])]
        for sr in range(2 * slots):
            lt[q][sr * lat_n : (sr + 1) * lat_n, :] = jnp.concatenate(
                [part[:, cl * sr : cl * (sr + 1)] for part in parts], axis=1
            )
        head = first_columns(q)
        turned = lt[q][...].T
        for low, high in ((0, head), (head, ptiles)):
            if low == high:
                continue
            grid = dot(turned, wv[:, 128 * low : 128 * high]).astype(BF16)
            for jj in range(nj):
                for k in range(low, high):
                    part = grid[cl * jj : cl * (jj + 1), 128 * (k - low) : 128 * (k - low + 1)]
                    g[q][flat(q, jj * ptiles + k)] = part
            if head < ptiles:
                start_points(q, 0 if low == 0 else 1)
        if head == ptiles:
            for n in range(slots_of(q)):
                start_points(q, n)
        start_own(q)

    for q, nj in enumerate(chunks):
        wait_points(q)
        drain_sent(q, nq + q, g[q])
        for n in range(0, slots_of(q), 2):
            tiles = range(n, min(n + 2, slots_of(q)))
            points = jnp.concatenate([r2[q][tile] for tile in tiles], axis=1)
            pre = dot(w_in[...], points)
            hidden = gelu(pre + jnp.concatenate([bias for _ in tiles], axis=1)).astype(BF16)
            mixed = (points.astype(F32) + dot(w_out[...], hidden)).astype(BF16)
            for dest in range(chan_n):
                for k, tile in enumerate(tiles):
                    mx[q][dest * slots_of(q) + tile] = mixed[cl * dest : cl * (dest + 1), 128 * k : 128 * (k + 1)]
        start_mixed(q)

    wvt[...] = wv[...].T

    for q, nj in enumerate(chunks):
        wait_mixed(q)
        field = []
        for jj in range(nj):
            tiles = [jj * ptiles + k for k in range(ptiles)]
            field.append(jnp.concatenate([r3[q][flat(q, tile)] for tile in tiles], axis=1))
        modes = dot(jnp.concatenate(field, axis=0), wvt[...]).astype(BF16).T
        for jj in range(nj):
            value = jnp.concatenate(
                [modes[lat_n * sr : lat_n * (sr + 1), cl * jj : cl * (jj + 1)] for sr in range(2 * slots)], axis=1
            )
            value = value.astype(F32)
            for k in range(ltiles):
                scr[q][k, pl.ds(jj, lat_n, stride=nj), :] = value[:, 128 * k : 128 * (k + 1)]
        s4[q][...] = message(q)
        start_lat(q, s4[q], r4[q], 3 * nq + q)

    def swap(a):
        low = (iota((a.shape[0], 128), 1) // cl) % 2 == 0
        pieces = []
        for k in range(ltiles):
            piece = a[:, 128 * k : 128 * (k + 1)]
            pieces.append(jnp.where(low, pltpu.roll(piece, 128 - cl, 1), pltpu.roll(piece, cl, 1)))
        return jnp.concatenate(pieces, axis=1)

    edge = min(16, lat_n * chunks[0])
    carried = None
    for q, nj in enumerate(chunks):
        wait_lat(q, s4[q], r4[q], 3 * nq + q)
        here = jnp.concatenate(unpack(q, r4[q]), axis=0)
        turned = swap(here)
        to_next, own, to_last = (direct[i] * here + crossed[i] * turned for i in range(3))
        n_rows = lat_n * nj
        row = iota((n_rows, 1), 0)
        from_last = half_turn * to_next[:1] if q == 0 else carried
        from_next = half_turn * to_last[n_rows - 1 :] if q == nq - 1 else jnp.zeros_like(from_last)
        carried = to_next[n_rows - 1 :]
        field = own + jnp.where(row == 0, from_last, pltpu.roll(to_next, 1, 0))
        field = field + jnp.where(row == n_rows - 1, from_next, pltpu.roll(to_last, n_rows - 1, 0))
        field = field.astype(BF16)
        start = first_row[q]
        if q > 0:
            missing = jnp.where(iota((edge, lanes_n), 0) == edge - 1, to_last[:1], 0.0).astype(BF16)
            field = jnp.concatenate([missing, field], axis=0)
            start -= edge
        span = slice(start, first_row[q] + n_rows)
        left = [
            dot(merge, field[:, first * cr : (first + pair) * cr], NT).astype(BF16) for first in range(0, slots, pair)
        ]
        products = [
            dot(left[s // pair][s % pair * cr : (s % pair + 1) * cr], lb[s, span]) for s in range(slots)
        ]
        for s in range(slots):
            part = products[s] if q == 0 else products[s] + acc[s]
            if q < nq - 1:
                acc[s] = part
            else:
                out_ref[s, 0] = part.astype(BF16).reshape(cl, 2, deg)


def block(cfg, table, spec_in, legendre, mode_slot, w_in, b_in, w_out, kernel):
    lat_n, chan_n, _ = cfg
    slots, batch, cl, _, deg = spec_in.shape
    rows = legendre.shape[1] // lat_n
    lanes_n = slots * 2 * cl
    n_modes = mode_slot.shape[0]
    ptiles = NLON // 128
    width = [-(-n * ptiles // chan_n) for n in CHUNKS]
    both = list(zip(CHUNKS, width))
    vm = pl.BlockSpec(memory_space=pltpu.VMEM)
    hbm = pl.BlockSpec(memory_space=pltpu.HBM)
    scratch = [
        pltpu.VMEM(legendre.shape, F32),
        pltpu.VMEM((slots, legendre.shape[1], deg), BF16),
        pltpu.VMEM((2, n_modes, NLON), BF16),
        pltpu.VMEM((ptiles, n_modes, 128), F32),
        pltpu.VMEM((2 * n_modes, NLON), BF16),
        pltpu.VMEM((NLON, 2 * n_modes), BF16),
        pltpu.VMEM((slots, 2 * cl, deg), F32),
        pltpu.VMEM(spec_in.shape, BF16),
        pltpu.SMEM(mode_slot.shape, jnp.int32),
        pltpu.VMEM(mode_slot.shape, jnp.int32),
        pltpu.VMEM(w_in.shape, BF16),
        pltpu.VMEM((1, b_in.shape[0]), F32),
        pltpu.VMEM(w_out.shape, BF16),
        pltpu.VMEM(kernel.shape[::-1], F32),
    ]
    message = lambda: [pltpu.VMEM((lat_n, n, lanes_n), BF16) for n in CHUNKS]
    scratch += [pltpu.VMEM((lanes_n // 128, lat_n * n, 128), F32) for n in CHUNKS]
    scratch += message() + message()
    scratch += [pltpu.VMEM((2 * n_modes, cl * n), BF16) for n in CHUNKS]
    scratch += [pltpu.VMEM((chan_n * t, cl, 128), BF16) for n, t in both]
    scratch += [pltpu.VMEM((t, chan_n * cl, 128), BF16) for n, t in both]
    scratch += [pltpu.VMEM((chan_n * t, cl, 128), BF16) for n, t in both]
    scratch += [pltpu.VMEM((chan_n * t, cl, 128), BF16) for n, t in both]
    scratch += message() + message()
    nq = len(CHUNKS)
    scratch += [
        pltpu.SemaphoreType.DMA((5,)),
        pltpu.SemaphoreType.DMA((2 * nq,)),
        pltpu.SemaphoreType.DMA((4 * nq,)),
        pltpu.SemaphoreType.DMA((nq,)),
    ]
    return pl.pallas_call(
        functools.partial(body, cfg),
        out_shape=pltpu.VMEM(spec_in.shape, BF16),
        in_specs=[hbm] * 8,
        out_specs=vm,
        scratch_shapes=scratch,
        compiler_params=pltpu.CompilerParams(
            collective_id=0, has_side_effects=True, vmem_limit_bytes=60 * 1024 * 1024
        ),
        name="spherical_block",
    )(
        spec_in, legendre, jnp.asarray(table, BF16), mode_slot, w_in,
        b_in.reshape(1, -1), w_out, kernel.T,
    )


def solution(mesh, grid3=GRID3, modes=384):
    in_specs = (
        P("lat", None, "chan", None, None),
        P("lat", None, None),
        P(),
        P(),
        P(),
        P(),
        P("chan", None),
    )
    out_specs = P("lat", None, "chan", None, None)
    cfg = (mesh.shape["lat"], mesh.shape["chan"], grid3)
    table = wave_constant(modes, NLON)
    return jax.shard_map(
        functools.partial(block, cfg, table), mesh=mesh, in_specs=in_specs, out_specs=out_specs, check_vma=False
    )
```

```python
import functools
import math

import jax
import jax.numpy as jnp
import numpy as np
from jax import lax
from jax.experimental import pallas as pl
from jax.experimental.pallas import tpu as pltpu
from jax.sharding import PartitionSpec as P

NLON = 768
MESH = pl.DeviceIdType.MESH
F32 = jnp.float32
BF16 = jnp.bfloat16
CHUNKS = (2, 2, 2)
GRID3 = (4, 8, 2)
NT = (((1,), (1,)), ((), ()))
TN = (((0,), (0,)), ((), ()))
NN = (((1,), (0,)), ((), ()))


def dot(a, b, dims=NN, precision=None):
    return lax.dot_general(a, b, dims, preferred_element_type=F32, precision=precision)


def gelu(x):
    a = math.sqrt(2.0 / math.pi)
    half = 0.5 * x
    return half + half * jnp.tanh(x * (a + (a * 0.044715) * (x * x)))


def far_first(k, size):
    if size == 1:
        return 0 * k
    return size // 2 + (1 - 2 * (k % 2)) * ((k + 1) // 2)


def wave_constant(modes, count):
    phase = (np.arange(modes)[:, None] * np.arange(count)[None, :]) % count
    angle = phase * (2.0 * math.pi / count)
    factor = count ** -0.5
    return np.stack([np.cos(angle) * factor, -np.sin(angle) * factor]).astype(np.float32)


def iota(shape, dim):
    return lax.broadcasted_iota(jnp.int32, shape, dim)


def body(cfg, x_ref, leg_ref, table_ref, mode_hbm, w_in_ref, b_ref, w_out_ref, kern_ref, out_ref,
         legv, lb, tab, wvf, wv, wvt, acc, xv, mode_ref, mode_row, w_in, b_in, w_out, kern, *rest):
    lat_n, chan_n, grid3 = cfg
    chunks = CHUNKS
    nq = len(chunks)
    slots, _, cl, _, deg = x_ref.shape
    rows = sum(chunks)
    lanes_n = slots * 2 * cl
    ltiles = lanes_n // 128
    dtiles = deg // 128
    ptiles = NLON // 128
    cr = 2 * cl
    chans = cl * chan_n
    rest = list(rest)
    take = lambda n: [rest.pop(0) for _ in range(n)]
    scr, s1, r1, lt, g, r2, mx, r3, s4, r4 = (take(nq) for _ in range(10))
    in_sem, sends, recvs, locs = rest

    lat = lax.axis_index("lat")
    chan = lax.axis_index("chan")

    first_row = [lat_n * sum(chunks[:q]) for q in range(nq)]
    leg_copies = []
    for q, nj in enumerate(chunks):
        rows_q = pl.ds(first_row[q], lat_n * nj)
        leg_copies.append(
            [pltpu.make_async_copy(leg_ref.at[s, rows_q], legv.at[s, rows_q], locs.at[q]) for s in range(slots)]
        )
    in_copies = [
        pltpu.make_async_copy(src, dst, in_sem.at[k] if k < 5 else sends.at[nq + k - 5])
        for k, (src, dst) in enumerate(
            [(x_ref, xv), (mode_hbm, mode_ref), (table_ref, tab), (mode_hbm, mode_row), (w_in_ref, w_in), (b_ref, b_in), (w_out_ref, w_out), (kern_ref, kern)]
        )
    ]
    barrier = pltpu.get_barrier_semaphore()

    nx, nz, nc = grid3
    here_x, here_z, here_c = lat // (nz * nc), (lat // nc) % nz, lat % nc
    peer_x = [((here_x + dx) % nx) * (nz * nc) for dx in range(nx)]
    peer_z = [((here_z + dz) % nz) * nc for dz in range(nz)]
    peer_c = [(here_c + dc) % nc for dc in range(nc)]
    steps = [(dx, dz, dc) for dx in range(nx) for dz in range(nz) for dc in range(nc)]
    steps.sort(key=lambda step: -min(step[0], nx - step[0]) - min(step[1], nz - step[1]))
    steps.remove((0, 0, 0))
    chan_peers = [(chan + far_first(k, chan_n)) % chan_n for k in range(chan_n - 1)]

    def each_lat(act):
        for dx, dz, dc in steps:
            act(peer_x[dx] + peer_z[dz] + peer_c[dc])

    in_copies[0].start()
    in_copies[1].start()
    for copy in leg_copies[0]:
        copy.start()

    each_lat(lambda peer: pl.semaphore_signal(barrier, inc=1, device_id={"lat": peer}, device_id_type=MESH))
    for peer in chan_peers:
        pl.semaphore_signal(barrier, inc=1, device_id={"chan": peer}, device_id_type=MESH)
    in_copies[2].start()
    for per in leg_copies[1:]:
        for copy in per:
            copy.start()
    for copy in in_copies[3:]:
        copy.start()

    def sent_sem(at):
        return sends.at[at % nq if at // nq in (0, 3) else nq + at % nq]

    def start_lat(q, src, dst, at):
        def one(peer):
            pltpu.make_async_remote_copy(
                src_ref=src.at[peer], dst_ref=dst.at[lat], send_sem=sent_sem(at), recv_sem=recvs.at[at],
                device_id={"lat": peer}, device_id_type=MESH,
            ).start()

        each_lat(one)
        pltpu.make_async_copy(src.at[lat], dst.at[lat], locs.at[at % nq]).start()

    def wait_lat(q, src, dst, at):
        pltpu.make_async_copy(src.at[lat], dst.at[lat], locs.at[at % nq]).wait()
        pltpu.make_async_remote_copy(
            src_ref=src.at[pl.ds(0, lat_n - 1)], dst_ref=dst.at[pl.ds(0, lat_n - 1)],
            send_sem=sent_sem(at), recv_sem=recvs.at[at], device_id={"lat": (lat + 1) % lat_n}, device_id_type=MESH,
        ).wait()

    col_x = iota((cr, cr), 1)
    row_x = iota((cr, cr), 0)
    split = (col_x == (row_x % cl) * 2 + row_x // cl).astype(BF16)
    pair = 128 // cr
    wide_col, wide_row = iota((128, 128), 1), iota((128, 128), 0)
    merge = (wide_col == wide_row // cr * cr + (wide_row % 2) * cl + wide_row % cr // 2).astype(BF16)

    def message(q):
        nj = chunks[q]
        value = jnp.concatenate([scr[q][k] for k in range(ltiles)], axis=1)
        return value.reshape(lat_n, nj, lanes_n).astype(BF16)

    def unpack(q, received):
        nj = chunks[q]
        value = received[...].astype(F32).reshape(lat_n * nj, lanes_n)
        for k in range(ltiles):
            scr[q][k] = value[:, 128 * k : 128 * (k + 1)]
        return [
            jnp.concatenate([scr[q][k, pl.ds(jj, lat_n, stride=nj), :] for k in range(ltiles)], axis=1)
            for jj in range(nj)
        ]

    in_copies[0].wait()
    in_copies[1].wait()
    modes_here = [mode_ref[lat * slots + s] for s in range(slots)]
    spectra = [dot(split, xv[s, 0].reshape(cr, deg)).astype(BF16) for s in range(slots)]
    for q, nj in enumerate(chunks):
        span = slice(first_row[q], first_row[q] + lat_n * nj)
        degree = iota((lat_n * nj, deg), 1)
        rows_q = pl.ds(first_row[q], lat_n * nj)
        pltpu.make_async_copy(leg_ref.at[:, rows_q], legv.at[:, rows_q], locs.at[q]).wait()
        masked = [jnp.where(degree >= modes_here[s], legv[s, span], 0.0).astype(BF16) for s in range(slots)]
        products = [dot(masked[s], spectra[s], NT) for s in range(slots)]
        for s in range(slots):
            lb[s, span] = masked[s]
        for first in range(0, slots, pair):
            both = jnp.concatenate(products[first : first + pair], axis=1)
            for jj in range(nj):
                scr[q][first // pair, pl.ds(jj, lat_n, stride=nj), :] = both[jj * lat_n : (jj + 1) * lat_n]
        s1[q][...] = message(q)
    pl.semaphore_wait(barrier, lat_n - 1 + chan_n - 1)
    for q in range(nq):
        start_lat(q, s1[q], r1[q], q)

    for copy in in_copies[2:]:
        copy.wait()
    n_modes = mode_row.shape[0]
    pick = (iota((n_modes, n_modes), 0) == mode_row[...].reshape(1, n_modes)).astype(BF16)
    for r in range(2):
        chosen = dot(pick, tab[r], TN)
        for k in range(ptiles):
            wvf[k] = chosen[:, 128 * k : 128 * (k + 1)]
        for s in range(slots):
            for k in range(ptiles):
                wv[(s * 2 + r) * lat_n : (s * 2 + r + 1) * lat_n, 128 * k : 128 * (k + 1)] = wvf[
                    k, pl.ds(s, lat_n, stride=slots), :
                ].astype(BF16)

    lane_all = iota((1, lanes_n), 1)
    mode_lane = jnp.zeros((1, lanes_n), jnp.int32)
    for s in range(slots):
        mode_lane = jnp.where(lane_all // cr == s, mode_ref[lat * slots + s], mode_lane)
    theta = mode_lane.astype(F32) * (2.0 * math.pi / NLON)
    cos_m, sin_m = jnp.cos(theta), jnp.sin(theta)
    half_turn = jnp.where(mode_lane % 2 == 0, 1.0, -1.0).astype(F32)
    spread = (iota((cl, lanes_n), 1) % cl == iota((cl, lanes_n), 0)).astype(F32)
    taps = dot(kern[...], spread, precision=lax.Precision.HIGHEST)
    part_sign = jnp.where((lane_all // cl) % 2 == 0, -1.0, 1.0).astype(F32)
    direct, crossed = [], []
    for i in range(3):
        left, mid, right = (taps[3 * i + n : 3 * i + n + 1] for n in range(3))
        direct.append((left + right) * cos_m + mid + (1.0 if i == 1 else 0.0))
        crossed.append((right - left) * sin_m * part_sign)

    bias = jnp.broadcast_to(b_in[...], (128, b_in.shape[1])).T

    def slots_of(q):
        return -(-chunks[q] * ptiles // chan_n)

    def exact_chan(q):
        return chunks[q] * ptiles - (slots_of(q) - 1) * chan_n

    def first_columns(q):
        nj = chunks[q]
        even = slots_of(q) == 2 and chan_n % nj == 0 and chan_n // nj < ptiles
        return chan_n // nj if even else ptiles

    def place(q, tile):
        head = first_columns(q)
        if head < ptiles:
            jj, k = tile // ptiles, tile % ptiles
            n, at = (0, jj * head + k) if k < head else (1, jj * (ptiles - head) + k - head)
        else:
            n, at = tile // chan_n, tile % chan_n
        if n == slots_of(q) - 1 and 2 * exact_chan(q) == chan_n:
            at = 2 * at + q % 2
        return at, n

    def is_full(q, who):
        if 2 * exact_chan(q) == chan_n:
            return who % 2 == q % 2
        return who < exact_chan(q)

    def flat(q, tile):
        at, n = place(q, tile)
        return at * slots_of(q) + n

    def start_points(q, n):
        at = nq + q
        columns = pl.ds(pl.multiple_of(chan * cl, cl), cl)

        def send(peer):
            pltpu.make_async_remote_copy(
                src_ref=g[q].at[peer * slots_of(q) + n], dst_ref=r2[q].at[n, columns], send_sem=sent_sem(at),
                recv_sem=recvs.at[at], device_id={"chan": peer}, device_id_type=MESH,
            ).start()

        for peer in chan_peers:
            if n < slots_of(q) - 1 or exact_chan(q) == chan_n:
                send(peer)
            else:
                pl.when(is_full(q, peer))(functools.partial(send, peer))

    def start_own(q):
        def own(size):
            pltpu.make_async_copy(
                g[q].at[pl.ds(chan * slots_of(q), size)],
                r2[q].at[pl.ds(0, size), pl.ds(pl.multiple_of(chan * cl, cl), cl)], locs.at[q],
            ).start()

        by_size(q, own)

    def by_size(q, act):
        n = slots_of(q)
        if exact_chan(q) == chan_n:
            act(n)
        else:

            @pl.when(is_full(q, chan))
            def _():
                act(n)

            @pl.when(jnp.logical_not(is_full(q, chan)))
            def _():
                act(n - 1)

    def wait_points(q):
        at = nq + q

        def act(size):
            span = (chan_n - 1) * cl
            pltpu.make_async_copy(
                g[q].at[pl.ds(chan * slots_of(q), size)],
                r2[q].at[pl.ds(0, size), pl.ds(pl.multiple_of(chan * cl, cl), cl)], locs.at[at % nq],
            ).wait()
            pltpu.make_async_remote_copy(
                src_ref=r2[q].at[pl.ds(0, size), pl.ds(0, span)], dst_ref=r2[q].at[pl.ds(0, size), pl.ds(0, span)],
                send_sem=sent_sem(at), recv_sem=recvs.at[at], device_id={"chan": (chan + 1) % chan_n}, device_id_type=MESH,
            ).wait_recv()

        by_size(q, act)

    def drain_sent(q, at, buffer):
        total = chunks[q] * ptiles

        def act(size):
            part = buffer.at[pl.ds(0, total - size)]
            pltpu.make_async_remote_copy(
                src_ref=part, dst_ref=part, send_sem=sent_sem(at), recv_sem=recvs.at[at],
                device_id={"chan": (chan + 1) % chan_n}, device_id_type=MESH,
            ).wait_send()

        by_size(q, act)

    def start_mixed(q):
        at = 2 * nq + q

        def act(size):
            for peer in chan_peers:
                pltpu.make_async_remote_copy(
                    src_ref=mx[q].at[pl.ds(peer * slots_of(q), size)], dst_ref=r3[q].at[pl.ds(chan * slots_of(q), size)],
                    send_sem=sent_sem(at), recv_sem=recvs.at[at], device_id={"chan": peer}, device_id_type=MESH,
                ).start()
            pltpu.make_async_copy(
                mx[q].at[pl.ds(chan * slots_of(q), size)], r3[q].at[pl.ds(chan * slots_of(q), size)], locs.at[at % nq]
            ).start()

        by_size(q, act)

    def wait_mixed(q):
        at = 2 * nq + q
        total = chunks[q] * ptiles

        def act(size):
            pltpu.make_async_copy(
                mx[q].at[pl.ds(chan * slots_of(q), size)], r3[q].at[pl.ds(chan * slots_of(q), size)], locs.at[at % nq]
            ).wait()
            peer = {"chan": (chan + 1) % chan_n}
            sent = mx[q].at[pl.ds(0, (chan_n - 1) * size)]
            pltpu.make_async_remote_copy(
                src_ref=sent, dst_ref=sent, send_sem=sent_sem(at), recv_sem=recvs.at[at], device_id=peer, device_id_type=MESH,
            ).wait_send()
            got = r3[q].at[pl.ds(0, total - size)]
            pltpu.make_async_remote_copy(
                src_ref=got, dst_ref=got, send_sem=sent_sem(at), recv_sem=recvs.at[at], device_id=peer, device_id_type=MESH,
            ).wait_recv()

        by_size(q, act)

    for q, nj in enumerate(chunks):
        wait_lat(q, s1[q], r1[q], q)
        parts = [part.astype(BF16) for part in unpack(q, r1[q])]
        for sr in range(2 * slots):
            lt[q][sr * lat_n : (sr + 1) * lat_n, :] = jnp.concatenate(
                [part[:, cl * sr : cl * (sr + 1)] for part in parts], axis=1
            )
        head = first_columns(q)
        turned = lt[q][...].T
        for low, high in ((0, head), (head, ptiles)):
            if low == high:
                continue
            grid = dot(turned, wv[:, 128 * low : 128 * high]).astype(BF16)
            for jj in range(nj):
                for k in range(low, high):
                    part = grid[cl * jj : cl * (jj + 1), 128 * (k - low) : 128 * (k - low + 1)]
                    g[q][flat(q, jj * ptiles + k)] = part
            if head < ptiles:
                start_points(q, 0 if low == 0 else 1)
        if head == ptiles:
            for n in range(slots_of(q)):
                start_points(q, n)
        start_own(q)

    for q, nj in enumerate(chunks):
        wait_points(q)
        drain_sent(q, nq + q, g[q])
        for n in range(0, slots_of(q), 2):
            tiles = range(n, min(n + 2, slots_of(q)))
            points = jnp.concatenate([r2[q][tile] for tile in tiles], axis=1)
            pre = dot(w_in[...], points)
            hidden = gelu(pre + jnp.concatenate([bias for _ in tiles], axis=1)).astype(BF16)
            mixed = (points.astype(F32) + dot(w_out[...], hidden)).astype(BF16)
            for dest in range(chan_n):
                for k, tile in enumerate(tiles):
                    mx[q][dest * slots_of(q) + tile] = mixed[cl * dest : cl * (dest + 1), 128 * k : 128 * (k + 1)]
        start_mixed(q)

    wvt[...] = wv[...].T

    for q, nj in enumerate(chunks):
        wait_mixed(q)
        field = []
        for jj in range(nj):
            tiles = [jj * ptiles + k for k in range(ptiles)]
            field.append(jnp.concatenate([r3[q][flat(q, tile)] for tile in tiles], axis=1))
        modes = dot(jnp.concatenate(field, axis=0), wvt[...]).astype(BF16).T
        for jj in range(nj):
            value = jnp.concatenate(
                [modes[lat_n * sr : lat_n * (sr + 1), cl * jj : cl * (jj + 1)] for sr in range(2 * slots)], axis=1
            )
            value = value.astype(F32)
            for k in range(ltiles):
                scr[q][k, pl.ds(jj, lat_n, stride=nj), :] = value[:, 128 * k : 128 * (k + 1)]
        s4[q][...] = message(q)
        start_lat(q, s4[q], r4[q], 3 * nq + q)

    def swap(a):
        low = (iota((a.shape[0], 128), 1) // cl) % 2 == 0
        pieces = []
        for k in range(ltiles):
            piece = a[:, 128 * k : 128 * (k + 1)]
            pieces.append(jnp.where(low, pltpu.roll(piece, 128 - cl, 1), pltpu.roll(piece, cl, 1)))
        return jnp.concatenate(pieces, axis=1)

    edge = min(16, lat_n * chunks[0])
    carried = None
    for q, nj in enumerate(chunks):
        wait_lat(q, s4[q], r4[q], 3 * nq + q)
        here = jnp.concatenate(unpack(q, r4[q]), axis=0)
        turned = swap(here)
        to_next, own, to_last = (direct[i] * here + crossed[i] * turned for i in range(3))
        n_rows = lat_n * nj
        row = iota((n_rows, 1), 0)
        from_last = half_turn * to_next[:1] if q == 0 else carried
        from_next = half_turn * to_last[n_rows - 1 :] if q == nq - 1 else jnp.zeros_like(from_last)
        carried = to_next[n_rows - 1 :]
        field = own + jnp.where(row == 0, from_last, pltpu.roll(to_next, 1, 0))
        field = field + jnp.where(row == n_rows - 1, from_next, pltpu.roll(to_last, n_rows - 1, 0))
        field = field.astype(BF16)
        start = first_row[q]
        if q > 0:
            missing = jnp.where(iota((edge, lanes_n), 0) == edge - 1, to_last[:1], 0.0).astype(BF16)
            field = jnp.concatenate([missing, field], axis=0)
            start -= edge
        span = slice(start, first_row[q] + n_rows)
        left = [
            dot(merge, field[:, first * cr : (first + pair) * cr], NT).astype(BF16) for first in range(0, slots, pair)
        ]
        products = [
            dot(left[s // pair][s % pair * cr : (s % pair + 1) * cr], lb[s, span]) for s in range(slots)
        ]
        for s in range(slots):
            part = products[s] if q == 0 else products[s] + acc[s]
            if q < nq - 1:
                acc[s] = part
            else:
                out_ref[s, 0] = part.astype(BF16).reshape(cl, 2, deg)


def block(cfg, table, spec_in, legendre, mode_slot, w_in, b_in, w_out, kernel):
    lat_n, chan_n, _ = cfg
    slots, batch, cl, _, deg = spec_in.shape
    rows = legendre.shape[1] // lat_n
    lanes_n = slots * 2 * cl
    n_modes = mode_slot.shape[0]
    ptiles = NLON // 128
    width = [-(-n * ptiles // chan_n) for n in CHUNKS]
    both = list(zip(CHUNKS, width))
    vm = pl.BlockSpec(memory_space=pltpu.VMEM)
    hbm = pl.BlockSpec(memory_space=pltpu.HBM)
    scratch = [
        pltpu.VMEM(legendre.shape, F32),
        pltpu.VMEM((slots, legendre.shape[1], deg), BF16),
        pltpu.VMEM((2, n_modes, NLON), BF16),
        pltpu.VMEM((ptiles, n_modes, 128), F32),
        pltpu.VMEM((2 * n_modes, NLON), BF16),
        pltpu.VMEM((NLON, 2 * n_modes), BF16),
        pltpu.VMEM((slots, 2 * cl, deg), F32),
        pltpu.VMEM(spec_in.shape, BF16),
        pltpu.SMEM(mode_slot.shape, jnp.int32),
        pltpu.VMEM(mode_slot.shape, jnp.int32),
        pltpu.VMEM(w_in.shape, BF16),
        pltpu.VMEM((1, b_in.shape[0]), F32),
        pltpu.VMEM(w_out.shape, BF16),
        pltpu.VMEM(kernel.shape[::-1], F32),
    ]
    message = lambda: [pltpu.VMEM((lat_n, n, lanes_n), BF16) for n in CHUNKS]
    scratch += [pltpu.VMEM((lanes_n // 128, lat_n * n, 128), F32) for n in CHUNKS]
    scratch += message() + message()
    scratch += [pltpu.VMEM((2 * n_modes, cl * n), BF16) for n in CHUNKS]
    scratch += [pltpu.VMEM((chan_n * t, cl, 128), BF16) for n, t in both]
    scratch += [pltpu.VMEM((t, chan_n * cl, 128), BF16) for n, t in both]
    scratch += [pltpu.VMEM((chan_n * t, cl, 128), BF16) for n, t in both]
    scratch += [pltpu.VMEM((chan_n * t, cl, 128), BF16) for n, t in both]
    scratch += message() + message()
    nq = len(CHUNKS)
    scratch += [
        pltpu.SemaphoreType.DMA((5,)),
        pltpu.SemaphoreType.DMA((2 * nq,)),
        pltpu.SemaphoreType.DMA((4 * nq,)),
        pltpu.SemaphoreType.DMA((nq,)),
    ]
    return pl.pallas_call(
        functools.partial(body, cfg),
        out_shape=pltpu.VMEM(spec_in.shape, BF16),
        in_specs=[hbm] * 8,
        out_specs=vm,
        scratch_shapes=scratch,
        compiler_params=pltpu.CompilerParams(
            collective_id=0, has_side_effects=True, vmem_limit_bytes=60 * 1024 * 1024
        ),
        name="spherical_block",
    )(
        spec_in, legendre, jnp.asarray(table, BF16), mode_slot, w_in,
        b_in.reshape(1, -1), w_out, kernel.T,
    )


def solution(mesh, grid3=GRID3, modes=384):
    in_specs = (
        P("lat", None, "chan", None, None),
        P("lat", None, None),
        P(),
        P(),
        P(),
        P(),
        P("chan", None),
    )
    out_specs = P("lat", None, "chan", None, None)
    cfg = (mesh.shape["lat"], mesh.shape["chan"], grid3)
    table = wave_constant(modes, NLON)
    return jax.shard_map(
        functools.partial(block, cfg, table), mesh=mesh, in_specs=in_specs, out_specs=out_specs, check_vma=False
    )
```

```python
import functools
import math

import jax
import jax.numpy as jnp
import numpy as np
from jax import lax
from jax.experimental import pallas as pl
from jax.experimental.pallas import tpu as pltpu
from jax.sharding import PartitionSpec as P

NLON = 768
MESH = pl.DeviceIdType.MESH
F32 = jnp.float32
BF16 = jnp.bfloat16
CHUNKS = (2, 2, 2)
GRID3 = (4, 8, 2)
NT = (((1,), (1,)), ((), ()))
TN = (((0,), (0,)), ((), ()))
NN = (((1,), (0,)), ((), ()))


def dot(a, b, dims=NN, precision=None):
    return lax.dot_general(a, b, dims, preferred_element_type=F32, precision=precision)


def far_first(k, size):
    if size == 1:
        return 0 * k
    return size // 2 + (1 - 2 * (k % 2)) * ((k + 1) // 2)


def wave_constant(modes, count):
    phase = (np.arange(modes)[:, None] * np.arange(count)[None, :]) % count
    angle = phase * (2.0 * math.pi / count)
    factor = count ** -0.5
    return np.stack([np.cos(angle) * factor, -np.sin(angle) * factor]).astype(np.float32)


def iota(shape, dim):
    return lax.broadcasted_iota(jnp.int32, shape, dim)


def body(cfg, x_ref, leg_ref, table_ref, mode_hbm, w_in_ref, b_ref, w_out_ref, kern_ref, out_ref,
         legv, lb, tab, wvf, wv, wvt, acc, xv, mode_ref, mode_row, w_in, b_in, w_out, kern, *rest):
    lat_n, chan_n, grid3 = cfg
    chunks = CHUNKS
    nq = len(chunks)
    slots, _, cl, _, deg = x_ref.shape
    rows = sum(chunks)
    lanes_n = slots * 2 * cl
    ltiles = lanes_n // 128
    dtiles = deg // 128
    ptiles = NLON // 128
    cr = 2 * cl
    chans = cl * chan_n
    rest = list(rest)
    take = lambda n: [rest.pop(0) for _ in range(n)]
    scr, s1, r1, lt, g, r2, mx, r3, s4, r4 = (take(nq) for _ in range(10))
    in_sem, sends, recvs, locs = rest

    lat = lax.axis_index("lat")
    chan = lax.axis_index("chan")

    first_row = [lat_n * sum(chunks[:q]) for q in range(nq)]
    leg_copies = []
    for q, nj in enumerate(chunks):
        rows_q = pl.ds(first_row[q], lat_n * nj)
        leg_copies.append(
            [pltpu.make_async_copy(leg_ref.at[s, rows_q], legv.at[s, rows_q], locs.at[q]) for s in range(slots)]
        )
    in_copies = [
        pltpu.make_async_copy(src, dst, in_sem.at[k] if k < 5 else sends.at[nq + k - 5])
        for k, (src, dst) in enumerate(
            [(x_ref, xv), (mode_hbm, mode_ref), (table_ref, tab), (mode_hbm, mode_row), (w_in_ref, w_in), (b_ref, b_in), (w_out_ref, w_out), (kern_ref, kern)]
        )
    ]
    barrier = pltpu.get_barrier_semaphore()

    nx, nz, nc = grid3
    here_x, here_z, here_c = lat // (nz * nc), (lat // nc) % nz, lat % nc
    peer_x = [((here_x + far_first(k, nx)) % nx) * (nz * nc) for k in range(nx)]
    peer_c = [(here_c + nc - 1 - k) % nc for k in range(nc)]
    peer_xc = [x + c for x in peer_x for c in peer_c]
    chan_peers = [(chan + far_first(k, chan_n)) % chan_n for k in range(chan_n - 1)]

    def each_lat(act):
        def at_z(k, carry):
            z = ((here_z + far_first(k, nz)) % nz) * nc
            for base in peer_xc:
                act(base + z)
            return carry

        lax.fori_loop(0, nz - 1, at_z, 0)
        for base in peer_xc[:-1]:
            act(base + here_z * nc)

    each_lat(lambda peer: pl.semaphore_signal(barrier, inc=1, device_id={"lat": peer}, device_id_type=MESH))
    for peer in chan_peers:
        pl.semaphore_signal(barrier, inc=1, device_id={"chan": peer}, device_id_type=MESH)
    in_copies[0].start()
    in_copies[1].start()
    for copy in leg_copies[0]:
        copy.start()
    in_copies[2].start()
    for per in leg_copies[1:]:
        for copy in per:
            copy.start()
    for copy in in_copies[3:]:
        copy.start()

    def sent_sem(at):
        return sends.at[at % nq if at // nq in (0, 3) else nq + at % nq]

    def start_lat(q, src, dst, at):
        def one(peer):
            pltpu.make_async_remote_copy(
                src_ref=src.at[peer], dst_ref=dst.at[lat], send_sem=sent_sem(at), recv_sem=recvs.at[at],
                device_id={"lat": peer}, device_id_type=MESH,
            ).start()

        each_lat(one)
        pltpu.make_async_copy(src.at[lat], dst.at[lat], locs.at[at % nq]).start()

    def wait_lat(q, src, dst, at):
        pltpu.make_async_copy(src.at[lat], dst.at[lat], locs.at[at % nq]).wait()
        pltpu.make_async_remote_copy(
            src_ref=src.at[pl.ds(0, lat_n - 1)], dst_ref=dst.at[pl.ds(0, lat_n - 1)],
            send_sem=sent_sem(at), recv_sem=recvs.at[at], device_id={"lat": (lat + 1) % lat_n}, device_id_type=MESH,
        ).wait()

    col_x = iota((cr, cr), 1)
    row_x = iota((cr, cr), 0)
    split = (col_x == (row_x % cl) * 2 + row_x // cl).astype(BF16)
    pair = 128 // cr
    wide_col, wide_row = iota((128, 128), 1), iota((128, 128), 0)
    merge = (wide_col == wide_row // cr * cr + (wide_row % 2) * cl + wide_row % cr // 2).astype(BF16)

    def message(q):
        nj = chunks[q]
        value = jnp.concatenate([scr[q][k] for k in range(ltiles)], axis=1)
        return value.reshape(lat_n, nj, lanes_n).astype(BF16)

    def unpack(q, received):
        nj = chunks[q]
        value = received[...].astype(F32).reshape(lat_n * nj, lanes_n)
        for k in range(ltiles):
            scr[q][k] = value[:, 128 * k : 128 * (k + 1)]
        return [
            jnp.concatenate([scr[q][k, pl.ds(jj, lat_n, stride=nj), :] for k in range(ltiles)], axis=1)
            for jj in range(nj)
        ]

    in_copies[0].wait()
    in_copies[1].wait()
    modes_here = [mode_ref[lat * slots + s] for s in range(slots)]
    spectra = [dot(split, xv[s, 0].reshape(cr, deg)).astype(BF16) for s in range(slots)]
    for q, nj in enumerate(chunks):
        span = slice(first_row[q], first_row[q] + lat_n * nj)
        degree = iota((lat_n * nj, deg), 1)
        rows_q = pl.ds(first_row[q], lat_n * nj)
        pltpu.make_async_copy(leg_ref.at[:, rows_q], legv.at[:, rows_q], locs.at[q]).wait()
        masked = [jnp.where(degree >= modes_here[s], legv[s, span], 0.0).astype(BF16) for s in range(slots)]
        products = [dot(masked[s], spectra[s], NT) for s in range(slots)]
        for s in range(slots):
            lb[s, span] = masked[s]
        for first in range(0, slots, pair):
            both = jnp.concatenate(products[first : first + pair], axis=1)
            for jj in range(nj):
                scr[q][first // pair, pl.ds(jj, lat_n, stride=nj), :] = both[jj * lat_n : (jj + 1) * lat_n]
        s1[q][...] = message(q)
    pl.semaphore_wait(barrier, lat_n - 1 + chan_n - 1)
    for q in range(nq):
        start_lat(q, s1[q], r1[q], q)

    for copy in in_copies[2:]:
        copy.wait()
    n_modes = mode_row.shape[0]
    pick = (iota((n_modes, n_modes), 0) == mode_row[...].reshape(1, n_modes)).astype(BF16)
    for r in range(2):
        chosen = dot(pick, tab[r], TN)
        for k in range(ptiles):
            wvf[k] = chosen[:, 128 * k : 128 * (k + 1)]
        for s in range(slots):
            for k in range(ptiles):
                wv[(s * 2 + r) * lat_n : (s * 2 + r + 1) * lat_n, 128 * k : 128 * (k + 1)] = wvf[
                    k, pl.ds(s, lat_n, stride=slots), :
                ].astype(BF16)

    lane_all = iota((1, lanes_n), 1)
    mode_lane = jnp.zeros((1, lanes_n), jnp.int32)
    for s in range(slots):
        mode_lane = jnp.where(lane_all // cr == s, mode_ref[lat * slots + s], mode_lane)
    theta = mode_lane.astype(F32) * (2.0 * math.pi / NLON)
    cos_m, sin_m = jnp.cos(theta), jnp.sin(theta)
    half_turn = jnp.where(mode_lane % 2 == 0, 1.0, -1.0).astype(F32)
    spread = (iota((cl, lanes_n), 1) % cl == iota((cl, lanes_n), 0)).astype(F32)
    taps = dot(kern[...], spread, precision=lax.Precision.HIGHEST)
    part_sign = jnp.where((lane_all // cl) % 2 == 0, -1.0, 1.0).astype(F32)
    direct, crossed = [], []
    for i in range(3):
        left, mid, right = (taps[3 * i + n : 3 * i + n + 1] for n in range(3))
        direct.append((left + right) * cos_m + mid + (1.0 if i == 1 else 0.0))
        crossed.append((right - left) * sin_m * part_sign)

    bias = jnp.broadcast_to(b_in[...], (128, b_in.shape[1])).T

    def slots_of(q):
        return -(-chunks[q] * ptiles // chan_n)

    def exact_chan(q):
        return chunks[q] * ptiles - (slots_of(q) - 1) * chan_n

    def place(q, tile):
        n, at = tile // chan_n, tile % chan_n
        if n == slots_of(q) - 1 and 2 * exact_chan(q) == chan_n:
            at = 2 * at + q % 2
        return at, n

    def is_full(q, who):
        if 2 * exact_chan(q) == chan_n:
            return who % 2 == q % 2
        return who < exact_chan(q)

    def flat(q, tile):
        at, n = place(q, tile)
        return at * slots_of(q) + n

    def chan_copies(q, src_of, dst_of, at):
        n = slots_of(q)
        even = exact_chan(q) == chan_n

        def run(act):
            for peer in chan_peers:
                count = lambda size: act(
                    pltpu.make_async_remote_copy(
                        src_ref=src_of(peer, size), dst_ref=dst_of(size), send_sem=sent_sem(at),
                        recv_sem=recvs.at[at], device_id={"chan": peer}, device_id_type=MESH,
                    )
                )
                if even:
                    count(n)
                else:
                    full = is_full(q, peer)

                    @pl.when(full)
                    def _():
                        count(n)

                    @pl.when(jnp.logical_not(full))
                    def _():
                        count(n - 1)

        return run

    def grid_src(q):
        return lambda peer, size: g[q].at[pl.ds(peer * slots_of(q), size)]

    def start_points(q):
        at = nq + q
        chan_copies(
            q, grid_src(q),
            lambda size: r2[q].at[pl.ds(0, size), pl.ds(pl.multiple_of(chan * cl, cl), cl)],
            at,
        )(lambda copy: copy.start())
        n = slots_of(q)

        def own(size):
            pltpu.make_async_copy(
                g[q].at[pl.ds(chan * slots_of(q), size)],
                r2[q].at[pl.ds(0, size), pl.ds(pl.multiple_of(chan * cl, cl), cl)], locs.at[at % nq],
            ).start()

        by_size(q, own)

    def by_size(q, act):
        n = slots_of(q)
        if exact_chan(q) == chan_n:
            act(n)
        else:

            @pl.when(is_full(q, chan))
            def _():
                act(n)

            @pl.when(jnp.logical_not(is_full(q, chan)))
            def _():
                act(n - 1)

    def wait_points(q):
        at = nq + q

        def act(size):
            span = (chan_n - 1) * cl
            pltpu.make_async_copy(
                g[q].at[pl.ds(chan * slots_of(q), size)],
                r2[q].at[pl.ds(0, size), pl.ds(pl.multiple_of(chan * cl, cl), cl)], locs.at[at % nq],
            ).wait()
            pltpu.make_async_remote_copy(
                src_ref=r2[q].at[pl.ds(0, size), pl.ds(0, span)], dst_ref=r2[q].at[pl.ds(0, size), pl.ds(0, span)],
                send_sem=sent_sem(at), recv_sem=recvs.at[at], device_id={"chan": (chan + 1) % chan_n}, device_id_type=MESH,
            ).wait_recv()

        by_size(q, act)

    def drain_sent(q, at, buffer):
        total = chunks[q] * ptiles

        def act(size):
            part = buffer.at[pl.ds(0, total - size)]
            pltpu.make_async_remote_copy(
                src_ref=part, dst_ref=part, send_sem=sent_sem(at), recv_sem=recvs.at[at],
                device_id={"chan": (chan + 1) % chan_n}, device_id_type=MESH,
            ).wait_send()

        by_size(q, act)

    def start_mixed(q):
        at = 2 * nq + q

        def act(size):
            for peer in chan_peers:
                pltpu.make_async_remote_copy(
                    src_ref=mx[q].at[pl.ds(peer * slots_of(q), size)], dst_ref=r3[q].at[pl.ds(chan * slots_of(q), size)],
                    send_sem=sent_sem(at), recv_sem=recvs.at[at], device_id={"chan": peer}, device_id_type=MESH,
                ).start()
            pltpu.make_async_copy(
                mx[q].at[pl.ds(chan * slots_of(q), size)], r3[q].at[pl.ds(chan * slots_of(q), size)], locs.at[at % nq]
            ).start()

        by_size(q, act)

    def wait_mixed(q):
        at = 2 * nq + q
        total = chunks[q] * ptiles

        def act(size):
            pltpu.make_async_copy(
                mx[q].at[pl.ds(chan * slots_of(q), size)], r3[q].at[pl.ds(chan * slots_of(q), size)], locs.at[at % nq]
            ).wait()
            peer = {"chan": (chan + 1) % chan_n}
            sent = mx[q].at[pl.ds(0, (chan_n - 1) * size)]
            pltpu.make_async_remote_copy(
                src_ref=sent, dst_ref=sent, send_sem=sent_sem(at), recv_sem=recvs.at[at], device_id=peer, device_id_type=MESH,
            ).wait_send()
            got = r3[q].at[pl.ds(0, total - size)]
            pltpu.make_async_remote_copy(
                src_ref=got, dst_ref=got, send_sem=sent_sem(at), recv_sem=recvs.at[at], device_id=peer, device_id_type=MESH,
            ).wait_recv()

        by_size(q, act)

    for q, nj in enumerate(chunks):
        wait_lat(q, s1[q], r1[q], q)
        parts = [part.astype(BF16) for part in unpack(q, r1[q])]
        for sr in range(2 * slots):
            lt[q][sr * lat_n : (sr + 1) * lat_n, :] = jnp.concatenate(
                [part[:, cl * sr : cl * (sr + 1)] for part in parts], axis=1
            )
        grid = dot(lt[q][...], wv[...], TN).astype(BF16)
        for jj in range(nj):
            for k in range(ptiles):
                tile = jj * ptiles + k
                g[q][flat(q, tile)] = grid[cl * jj : cl * (jj + 1), 128 * k : 128 * (k + 1)]
        start_points(q)

    for q, nj in enumerate(chunks):
        wait_points(q)
        drain_sent(q, nq + q, g[q])
        for n in range(0, slots_of(q), 2):
            tiles = range(n, min(n + 2, slots_of(q)))
            points = jnp.concatenate([r2[q][tile] for tile in tiles], axis=1)
            pre = dot(w_in[...], points)
            hidden = jax.nn.gelu(pre + jnp.concatenate([bias for _ in tiles], axis=1), approximate=True).astype(BF16)
            mixed = (points.astype(F32) + dot(w_out[...], hidden)).astype(BF16)
            for dest in range(chan_n):
                for k, tile in enumerate(tiles):
                    mx[q][dest * slots_of(q) + tile] = mixed[cl * dest : cl * (dest + 1), 128 * k : 128 * (k + 1)]
        start_mixed(q)

    wvt[...] = wv[...].T

    for q, nj in enumerate(chunks):
        wait_mixed(q)
        field = []
        for jj in range(nj):
            tiles = [jj * ptiles + k for k in range(ptiles)]
            field.append(jnp.concatenate([r3[q][flat(q, tile)] for tile in tiles], axis=1))
        modes = dot(jnp.concatenate(field, axis=0), wvt[...]).T
        for jj in range(nj):
            value = jnp.concatenate(
                [modes[lat_n * sr : lat_n * (sr + 1), cl * jj : cl * (jj + 1)] for sr in range(2 * slots)], axis=1
            )
            for k in range(ltiles):
                scr[q][k, pl.ds(jj, lat_n, stride=nj), :] = value[:, 128 * k : 128 * (k + 1)]
        s4[q][...] = message(q)
        start_lat(q, s4[q], r4[q], 3 * nq + q)

    def swap(a):
        low = (iota((a.shape[0], 128), 1) // cl) % 2 == 0
        pieces = []
        for k in range(ltiles):
            piece = a[:, 128 * k : 128 * (k + 1)]
            pieces.append(jnp.where(low, pltpu.roll(piece, 128 - cl, 1), pltpu.roll(piece, cl, 1)))
        return jnp.concatenate(pieces, axis=1)

    edge = min(16, lat_n * chunks[0])
    carried = None
    for q, nj in enumerate(chunks):
        wait_lat(q, s4[q], r4[q], 3 * nq + q)
        here = jnp.concatenate(unpack(q, r4[q]), axis=0)
        turned = swap(here)
        to_next, own, to_last = (direct[i] * here + crossed[i] * turned for i in range(3))
        n_rows = lat_n * nj
        row = iota((n_rows, 1), 0)
        from_last = half_turn * to_next[:1] if q == 0 else carried
        from_next = half_turn * to_last[n_rows - 1 :] if q == nq - 1 else jnp.zeros_like(from_last)
        carried = to_next[n_rows - 1 :]
        field = own + jnp.where(row == 0, from_last, pltpu.roll(to_next, 1, 0))
        field = field + jnp.where(row == n_rows - 1, from_next, pltpu.roll(to_last, n_rows - 1, 0))
        field = field.astype(BF16)
        start = first_row[q]
        if q > 0:
            missing = jnp.where(iota((edge, lanes_n), 0) == edge - 1, to_last[:1], 0.0).astype(BF16)
            field = jnp.concatenate([missing, field], axis=0)
            start -= edge
        span = slice(start, first_row[q] + n_rows)
        left = [
            dot(merge, field[:, first * cr : (first + pair) * cr], NT).astype(BF16) for first in range(0, slots, pair)
        ]
        products = [
            dot(left[s // pair][s % pair * cr : (s % pair + 1) * cr], lb[s, span]) for s in range(slots)
        ]
        for s in range(slots):
            part = products[s] if q == 0 else products[s] + acc[s]
            if q < nq - 1:
                acc[s] = part
            else:
                out_ref[s, 0] = part.astype(BF16).reshape(cl, 2, deg)


def block(cfg, table, spec_in, legendre, mode_slot, w_in, b_in, w_out, kernel):
    lat_n, chan_n, _ = cfg
    slots, batch, cl, _, deg = spec_in.shape
    rows = legendre.shape[1] // lat_n
    lanes_n = slots * 2 * cl
    n_modes = mode_slot.shape[0]
    ptiles = NLON // 128
    width = [-(-n * ptiles // chan_n) for n in CHUNKS]
    both = list(zip(CHUNKS, width))
    vm = pl.BlockSpec(memory_space=pltpu.VMEM)
    hbm = pl.BlockSpec(memory_space=pltpu.HBM)
    scratch = [
        pltpu.VMEM(legendre.shape, F32),
        pltpu.VMEM((slots, legendre.shape[1], deg), BF16),
        pltpu.VMEM((2, n_modes, NLON), BF16),
        pltpu.VMEM((ptiles, n_modes, 128), F32),
        pltpu.VMEM((2 * n_modes, NLON), BF16),
        pltpu.VMEM((NLON, 2 * n_modes), BF16),
        pltpu.VMEM((slots, 2 * cl, deg), F32),
        pltpu.VMEM(spec_in.shape, BF16),
        pltpu.SMEM(mode_slot.shape, jnp.int32),
        pltpu.VMEM(mode_slot.shape, jnp.int32),
        pltpu.VMEM(w_in.shape, BF16),
        pltpu.VMEM((1, b_in.shape[0]), F32),
        pltpu.VMEM(w_out.shape, BF16),
        pltpu.VMEM(kernel.shape[::-1], F32),
    ]
    message = lambda: [pltpu.VMEM((lat_n, n, lanes_n), BF16) for n in CHUNKS]
    scratch += [pltpu.VMEM((lanes_n // 128, lat_n * n, 128), F32) for n in CHUNKS]
    scratch += message() + message()
    scratch += [pltpu.VMEM((2 * n_modes, cl * n), BF16) for n in CHUNKS]
    scratch += [pltpu.VMEM((chan_n * t, cl, 128), BF16) for n, t in both]
    scratch += [pltpu.VMEM((t, chan_n * cl, 128), BF16) for n, t in both]
    scratch += [pltpu.VMEM((chan_n * t, cl, 128), BF16) for n, t in both]
    scratch += [pltpu.VMEM((chan_n * t, cl, 128), BF16) for n, t in both]
    scratch += message() + message()
    nq = len(CHUNKS)
    scratch += [
        pltpu.SemaphoreType.DMA((5,)),
        pltpu.SemaphoreType.DMA((2 * nq,)),
        pltpu.SemaphoreType.DMA((4 * nq,)),
        pltpu.SemaphoreType.DMA((nq,)),
    ]
    return pl.pallas_call(
        functools.partial(body, cfg),
        out_shape=pltpu.VMEM(spec_in.shape, BF16),
        in_specs=[hbm] * 8,
        out_specs=vm,
        scratch_shapes=scratch,
        compiler_params=pltpu.CompilerParams(
            collective_id=0, has_side_effects=True, vmem_limit_bytes=60 * 1024 * 1024
        ),
        name="spherical_block",
    )(
        spec_in, legendre, jnp.asarray(table, BF16), mode_slot, w_in,
        b_in.reshape(1, -1), w_out, kernel.T,
    )


def solution(mesh, grid3=GRID3, modes=384):
    in_specs = (
        P("lat", None, "chan", None, None),
        P("lat", None, None),
        P(),
        P(),
        P(),
        P(),
        P("chan", None),
    )
    out_specs = P("lat", None, "chan", None, None)
    cfg = (mesh.shape["lat"], mesh.shape["chan"], grid3)
    table = wave_constant(modes, NLON)
    return jax.shard_map(
        functools.partial(block, cfg, table), mesh=mesh, in_specs=in_specs, out_specs=out_specs, check_vma=False
    )
```
